32 devices in a mesh: station: 2 (over x), tm: 16 (over z, y, core).
Axes of the slice: x: 2, y: 2, z: 4, core: 2. Of those that a mesh axis runs over, the one named last changes fastest.
Arguments:
- spectra: float32 [512, 4, 4096], P('tm', 'station'), parts along dimension 1, may hold values from -6 to 6
- synth_taps: float32 [16, 512], replicated, may hold values from -1.5 to 1.5
- analysis_taps: float32 [16, 512], replicated, may hold values from -1.5 to 1.5
Outputs:
- channels: float32 [512, 4, 5120], P('tm', 'station'), parts along dimension 1
The draws below stay inside these ranges and needn't reach their ends.
There are 2 independent parts, one for each index of `station`. The reference program is written for one: setup_inputs(seed, part) draws one part's arguments, and reference() takes and returns one part's arrays. A program takes and returns all parts, laid end to end along the dimension named above; an argument that names none is the same for every part. Nothing has to cross between parts.
All inputs are finite; a program needn't handle non-finite values.
Results may differ from the reference program's by a relative error of at most 0.00007.
Values sent between devices are 32-bit elements; how exact they have to be, the bound alone decides.
No kernel may reach another device: no remote copies, remote signals or barrier semaphores. Data moves between devices by JAX's collectives and lax.ppermute only.
A program may use at most 64 MiB of HBM per device.

```python
import math
import jax
import jax.numpy as jnp
from jax import lax

M = 512
P_SIZE = 16
RT = 32
PHASES = 64
FRAMES = 4096


def block_scale(own_key, extent, shards, low, top_value):
    def one(dim, shards_of):
        heights = jax.random.uniform(jax.random.fold_in(jax.random.fold_in(own_key, 6), dim), (shards_of,), jnp.float32, low / len(shards), top_value / len(shards))
        return jnp.repeat(jnp.exp(heights), extent[dim] // shards_of).reshape((-1,) + (1,) * (len(extent) - dim - 1))

    factor_of = one(*shards[0])
    for cut in shards[1:]:
        factor_of = factor_of * one(*cut)
    return factor_of


def noise(own_key, extent, scale, reach, shards=(), kind=jnp.bfloat16):
    values = scale * jax.random.normal(own_key, extent, jnp.float32)
    if shards:
        values = values * block_scale(own_key, extent, shards, -0.22, 0.18)
    return jnp.clip(values, -reach, reach).astype(kind)


def setup_inputs(seed: int = 0, part: int = 0) -> dict:
    arg_keys = jax.random.split(jax.random.key(seed), 4)
    part_splits = jax.random.split(jax.random.fold_in(arg_keys[3], part), 4)
    spectra = noise(part_splits[0], (M, 2, FRAMES), 1.0, 6.0, ((0, 16),), jnp.float32)
    synth_taps = noise(arg_keys[1], (P_SIZE, M), P_SIZE ** -0.5, 1.5, (), jnp.float32)
    analysis_taps = noise(arg_keys[2], (P_SIZE, M), P_SIZE ** -0.5, 1.5, (), jnp.float32)
    return {"spectra": spectra, "synth_taps": synth_taps, "analysis_taps": analysis_taps}


def tables(width):
    index = jnp.arange(width, dtype=jnp.int32)
    product = index[:, None] * index[None, :] % width
    angle = product.astype(jnp.float32) * (2.0 * math.pi / width)
    scale = 1.0 / math.sqrt(width)
    return (jnp.cos(angle) * scale, jnp.sin(angle) * scale)

def resampler(width, taps_len, phases):
    out_width = 5 * width // 4
    sample = jnp.arange(out_width, dtype=jnp.int32)[:, None]
    column = jnp.arange(2 * width, dtype=jnp.int32)[None, :]
    start = 4 * sample // 5
    phase = phases * (4 * sample % 5) // 5
    lag = start + width - column
    offset = lag.astype(jnp.float32) + phase.astype(jnp.float32) / phases - (taps_len // 2 - 1)
    window = 0.5 + 0.5 * jnp.cos(math.pi * offset / (taps_len / 2.0))
    coeff = 0.9 * jnp.sinc(0.9 * offset) * window
    valid = (lag >= 0) & (lag < taps_len)
    full = jnp.where(valid, coeff, jnp.zeros_like(coeff))
    return (full[:, width:], full[:, :width])

def inverse(raw, cosines, sines):
    dims = (((0,), (0,)), ((), ()))
    with_cos = lax.dot_general(raw, cosines, dims, precision=lax.Precision.HIGHEST, preferred_element_type=jnp.float32)
    with_sin = lax.dot_general(raw, sines, dims, precision=lax.Precision.HIGHEST, preferred_element_type=jnp.float32)
    return jnp.stack([with_cos[0] - with_sin[1], with_sin[0] + with_cos[1]])

def forward(frames, cosines, sines):
    dims = (((1,), (2,)), ((), ()))
    with_cos = lax.dot_general(cosines, frames, dims, precision=lax.Precision.HIGHEST, preferred_element_type=jnp.float32)
    with_sin = lax.dot_general(sines, frames, dims, precision=lax.Precision.HIGHEST, preferred_element_type=jnp.float32)
    return jnp.stack([with_cos[:, 0] + with_sin[:, 1], with_cos[:, 1] - with_sin[:, 0]], axis=1)

def filtered(frames, taps):
    count = frames.shape[1] - taps.shape[0] + 1
    total = jnp.zeros((2, count, frames.shape[2]), frames.dtype)
    for lag_index in range(taps.shape[0]):
        first = taps.shape[0] - 1 - lag_index
        total = total + taps[lag_index][None, None, :] * frames[:, first:first + count]
    return total

def resample(stream, current, previous):
    width = stream.shape[2]
    now_rows = stream[:, 1:].reshape(-1, width)
    before_rows = stream[:, :-1].reshape(-1, width)
    dims = (((1,), (1,)), ((), ()))
    out = lax.dot_general(now_rows, current, dims, precision=lax.Precision.HIGHEST, preferred_element_type=jnp.float32)
    out = out + lax.dot_general(before_rows, previous, dims, precision=lax.Precision.HIGHEST, preferred_element_type=jnp.float32)
    return out.reshape(2, -1, width)

def reference(spectra, synth_taps, analysis_taps):
    cosines, sines = tables(M)
    current, previous = resampler(M, RT, PHASES)
    spread = inverse(spectra, cosines, sines)
    padded = jnp.concatenate([jnp.zeros((2, P_SIZE - 1, M), spread.dtype), spread], axis=1)
    stream = filtered(padded, synth_taps)
    stream = jnp.concatenate([jnp.zeros((2, 1, M), stream.dtype), stream], axis=1)
    resampled = resample(stream, current, previous)
    resampled = jnp.concatenate([jnp.zeros((2, P_SIZE - 1, M), resampled.dtype), resampled], axis=1)
    windowed = filtered(resampled, analysis_taps)
    return forward(windowed, cosines, sines)
```

```python
import functools
import math

import jax
import jax.numpy as jnp
import numpy as np
from jax import lax
from jax.experimental import pallas as pl
from jax.experimental.pallas import tpu as pltpu
from jax.sharding import PartitionSpec as P

RT = 32
PHASES = 64
UP, DOWN = 5, 4
LANES = 128
SUB = 8
HALO = 32


def split(value):
    high = value.astype(jnp.bfloat16)
    low = (value - high.astype(jnp.float32)).astype(jnp.bfloat16)
    return high, low


def np_split(value):
    value = value.astype(np.float32)
    high = value.astype(jnp.bfloat16)
    low = (value - high.astype(np.float32)).astype(jnp.bfloat16)
    return high, low


def radix4_tables(width):
    quarter = width // 4
    k = np.arange(quarter)[:, None]
    m = np.arange(quarter)[None, :]
    blocks = []
    for r in range(4):
        angle = ((4 * k + r) * m % width) * (2.0 * math.pi / width)
        cosine = np.cos(angle) / math.sqrt(width)
        sine = np.sin(angle) / math.sqrt(width)
        blocks.append(np.block([[cosine, sine], [-sine, cosine]]))
    return np_split(np.stack(blocks))


def resampler_tables():
    parts = []
    for j in range(UP):
        sample = np.arange(LANES)[None, :] + LANES * j
        start = 128 * (min(j, 3) - 1)
        column = np.arange(2 * LANES)[:, None] + start
        lag = DOWN * sample // UP - column
        phase = PHASES * (DOWN * sample % UP) // UP
        offset = lag + phase / PHASES - (RT // 2 - 1)
        window = 0.5 + 0.5 * np.cos(math.pi * offset / (RT / 2.0))
        coeff = 0.9 * np.sinc(0.9 * offset) * window
        parts.append(np_split(np.where((lag >= 0) & (lag < RT), coeff, 0.0)))
    out = [np.concatenate([high, low], axis=1) for high, low in parts[:3]]
    out.append(np.concatenate([parts[3][0], parts[4][0]], axis=1))
    out.append(np.concatenate([parts[3][1], parts[4][1]], axis=1))
    return np.stack(out)


def lane_iota():
    return lax.broadcasted_iota(jnp.int32, (SUB, LANES), 1)


def prep_kernel(order, blocks, x_ref, o_ref):
    stride = x_ref.shape[0] // (4 * SUB)
    lane = lane_iota()

    def tile(r, k, part):
        return x_ref[pl.ds(r * stride + 2 * k + part, SUB, stride=4 * stride), :]

    for place, dev in enumerate(order):
        for r in range(4):
            for lb in range(blocks):
                for part in range(2):
                    t = (r * blocks + lb) * 2 + part
                    o_ref[place, t * SUB : (t + 1) * SUB, :] = tile(r, blocks * dev + lb, part)
        for part in range(2):
            total = jnp.zeros((SUB, LANES), jnp.float32)
            if dev > 0:
                for r in range(4):
                    value = tile(r, blocks * dev - 1, part)
                    if r < 3:
                        value = pltpu.roll(value, HALO * (r + 1), 1)
                    total = jnp.where(lane // HALO == r, value, total)
            t = 8 * blocks + part
            o_ref[place, t * SUB : (t + 1) * SUB, :] = total


def main_kernel(
    order, frames, x_ref, w_hi, w_lo, res_ref, st_ref, at_ref, o_ref,
    a_ref, v_ref, y_ref, yh_ref, yl_ref, z_ref, u_ref, bh_ref, bl_ref,
):
    blocks = frames // LANES
    count = len(order)
    place_of = {dev: place for place, dev in enumerate(order)}
    f32 = jnp.float32

    def dot(a, b):
        return lax.dot_general(a, b, (((1,), (0,)), ((), ())), preferred_element_type=f32)

    def dot_t(a, b):
        return lax.dot_general(a, b, (((1,), (1,)), ((), ())), preferred_element_type=f32)

    def tile(t):
        return jnp.concatenate(
            [x_ref[place_of[s], t * SUB : (t + 1) * SUB, :] for s in range(count)], axis=0
        )

    halo = [tile(8 * blocks + part).T for part in range(2)]
    for r in range(4):
        rows = [jnp.concatenate([h[r * HALO : (r + 1) * HALO] for h in halo], axis=1)]
        for lb in range(blocks):
            rows.append(
                jnp.concatenate([tile((r * blocks + lb) * 2 + part).T for part in range(2)], axis=1)
            )
        high, low = split(jnp.concatenate(rows, axis=0))
        a_ref[r] = dot(high, w_hi[r]) + dot(low, w_hi[r]) + dot(high, w_lo[r])

    total = frames + HALO

    @pl.loop(0, total // 16)
    def _(i):
        row = pl.ds(pl.multiple_of(i * 16, 16), 16)
        re = [a_ref[r, row, :LANES] for r in range(4)]
        im = [a_ref[r, row, LANES:] for r in range(4)]
        sr, dr = re[0] + re[2], re[0] - re[2]
        si, di = im[0] + im[2], im[0] - im[2]
        tr, er = re[1] + re[3], re[1] - re[3]
        ti, ei = im[1] + im[3], im[1] - im[3]
        v_ref[0, row, :] = sr + tr
        v_ref[4, row, :] = si + ti
        v_ref[1, row, :] = dr - ei
        v_ref[5, row, :] = di + er
        v_ref[2, row, :] = sr - tr
        v_ref[6, row, :] = si - ti
        v_ref[3, row, :] = dr + ei
        v_ref[7, row, :] = di - er

    for k in range(8):
        v_ref[k, total : total + 16, :] = jnp.zeros((16, LANES), f32)
        y_ref[k * 2, 0:SUB, :] = jnp.zeros((SUB, LANES), f32)
        y_ref[k * 2 + 1, 0:SUB, :] = jnp.zeros((SUB, LANES), f32)
        y_ref[16 + k * 2, 0:SUB, :] = jnp.zeros((SUB, LANES), f32)
        y_ref[16 + k * 2 + 1, 0:SUB, :] = jnp.zeros((SUB, LANES), f32)

    taps_len = st_ref.shape[0]
    groups = (total // 4 - 4 + SUB) // SUB
    for q in range(4):
        taps = [
            jnp.broadcast_to(st_ref[p : p + 1, q * LANES : (q + 1) * LANES], (SUB, LANES))
            for p in range(taps_len)
        ]

        @pl.loop(0, 2 * groups)
        def _(i):
            part = i // groups
            t = i - part * groups
            base = t * 32 + 16
            vals = {
                j: v_ref[part * 4 + q, pl.ds(base + j, SUB, stride=4), :]
                for j in range(1 - taps_len, 4)
            }
            for b in range(4):
                acc = taps[0] * vals[b]
                for p in range(1, taps_len):
                    acc = acc + taps[p] * vals[b - p]
                y_ref[part * 16 + b * 4 + q, pl.ds(pl.multiple_of(t * SUB, SUB) + SUB, SUB), :] = acc

    rows = groups * SUB
    both = 2 * rows
    for b in range(4):
        for q in range(4):
            value = jnp.concatenate(
                [y_ref[part * 16 + b * 4 + q, SUB : SUB + rows, :] for part in range(2)], axis=0
            )
            high, low = split(value)
            first = b * both + (both if q == 3 else 0)
            yh_ref[q, first : first + both, :] = high
            yl_ref[q, first : first + both, :] = low
    value = jnp.concatenate(
        [y_ref[part * 16 + 15, SUB - 1 : SUB - 1 + rows, :] for part in range(2)], axis=0
    )
    high, low = split(value)
    yh_ref[3, 0:both, :] = high
    yl_ref[3, 0:both, :] = low

    def store_z(j, value):
        for b in range(4):
            g, q = (5 * b + j) // 4, (5 * b + j) % 4
            for part in range(2):
                first = b * both + part * rows
                z_ref[part * 20 + g * 4 + q] = value[first : first + rows]

    def pair(ref, left, right):
        first = both if left == 2 else 0
        a = ref[3, 0 : 4 * both] if left < 0 else ref[left, 0 : 4 * both]
        return jnp.concatenate([a, ref[right, first if right == 3 else 0 : (first if right == 3 else 0) + 4 * both]], axis=1)

    for j in range(3):
        high = pair(yh_ref, j - 1, j)
        low = pair(yl_ref, j - 1, j)
        wide = dot(high, res_ref[j])
        store_z(j, wide[:, :LANES] + wide[:, LANES:] + dot(low, res_ref[j, :, :LANES]))
    high = pair(yh_ref, 2, 3)
    low = pair(yl_ref, 2, 3)
    wide = dot(high, res_ref[3]) + dot(high, res_ref[4]) + dot(low, res_ref[3])
    store_z(3, wide[:, :LANES])
    store_z(4, wide[:, LANES:])

    outs = frames * UP // DOWN
    taps_len = at_ref.shape[0]
    groups2 = frames // 4 // SUB
    for q in range(4):
        taps = [
            jnp.broadcast_to(at_ref[p : p + 1, q * LANES : (q + 1) * LANES], (SUB, LANES))
            for p in range(taps_len)
        ]

        @pl.loop(0, 2 * groups2)
        def _(i):
            part = i // groups2
            t = i - part * groups2
            vals = {}
            for j in range(1 - taps_len, UP):
                shift = j // UP
                vals[j] = z_ref[part * 20 + (j - UP * shift) * 4 + q, pl.ds(t * SUB + 4 + shift, SUB), :]
            for g in range(UP):
                acc = taps[0] * vals[g]
                for p in range(1, taps_len):
                    acc = acc + taps[p] * vals[g - p]
                u_ref[part * 4 + q, pl.ds(t * SUB * UP + g, SUB, stride=UP), :] = acc

    @pl.loop(0, outs // 16)
    def _(i):
        row = pl.ds(pl.multiple_of(i * 16, 16), 16)
        re = [u_ref[q, row, :] for q in range(4)]
        im = [u_ref[4 + q, row, :] for q in range(4)]
        sr, dr = re[0] + re[2], re[0] - re[2]
        si, di = im[0] + im[2], im[0] - im[2]
        tr, er = re[1] + re[3], re[1] - re[3]
        ti, ei = im[1] + im[3], im[1] - im[3]
        spectra = [
            (sr + tr, si + ti), (dr + ei, di - er), (sr - tr, si - ti), (dr - ei, di + er)
        ]
        for r in range(4):
            for part in range(2):
                high, low = split(spectra[r][part])
                cols = slice(part * LANES, (part + 1) * LANES)
                bh_ref[r, row, cols] = high
                bl_ref[r, row, cols] = low

    lane = lax.broadcasted_iota(jnp.int32, (LANES, LANES), 1)
    full = outs // LANES
    rest = outs - full * LANES
    for r in range(4):
        for ref in (bh_ref, bl_ref):
            ref[r, outs : outs + rest] = ref[r, outs - rest : outs]
        high, low = bh_ref[r], bl_ref[r]
        out = dot_t(w_hi[r], high) + dot_t(w_hi[r], low) + dot_t(w_lo[r], high)
        for part in range(2):
            for k in range(full):
                t = k * SUB + r * 2 + part
                value = out[part * LANES : (part + 1) * LANES, k * LANES : (k + 1) * LANES]
                for place, dev in enumerate(order):
                    o_ref[place, t * SUB : (t + 1) * SUB, :] = value[dev * SUB : (dev + 1) * SUB]
        value = jnp.where(
            lane < rest, out[:LANES, full * LANES :], out[LANES:, full * LANES :]
        )
        t = full * SUB + r
        for place, dev in enumerate(order):
            o_ref[place, t * SUB : (t + 1) * SUB, :] = value[dev * SUB : (dev + 1) * SUB]


def final_kernel(order, x_ref, o_ref):
    stride = o_ref.shape[0] // (4 * SUB)
    lane = lane_iota()
    half = LANES // 2
    place_of = {dev: place for place, dev in enumerate(order)}

    def tile(dev, t):
        return x_ref[place_of[dev], t * SUB : (t + 1) * SUB, :]

    for dev in range(0, len(order), 2):
        for r in range(4):
            for part in range(2):
                t = r * 2 + part
                ends = [tile(dev, 16 + r), tile(dev + 1, 16 + r)]
                ends[1 - part] = pltpu.roll(ends[1 - part], half, 1)
                r0 = pltpu.roll(tile(dev + 1, t), half, 1)
                r1 = pltpu.roll(tile(dev + 1, 8 + t), half, 1)
                values = [
                    tile(dev, t),
                    tile(dev, 8 + t),
                    jnp.where(lane < half, ends[0], r0),
                    jnp.where(lane < half, r0, r1),
                    jnp.where(lane < half, r1, ends[1]),
                ]
                for k, value in enumerate(values):
                    first = r * stride + (5 * (dev // 2) + k) * 2 + part
                    o_ref[pl.ds(first, SUB, stride=4 * stride), :] = value


def shards(order, spectra, synth_taps, analysis_taps):
    count = lax.axis_size("tm")
    channels, parts, length = spectra.shape
    width = channels * count
    frames = length // count
    outs = frames * UP // DOWN
    blocks = frames // LANES
    order = tuple(order)
    groups = [list(order)]
    tiled = channels == 4 * SUB
    vmem = pl.BlockSpec(memory_space=pltpu.VMEM)
    f32, bf16 = jnp.float32, jnp.bfloat16
    rows_in = 8 * blocks * SUB + 2 * SUB
    rows_out = (outs * 64) // LANES
    sub = channels // 4

    def exchange(value):
        return lax.all_to_all(
            value, "tm", split_axis=0, concat_axis=0, tiled=True, axis_index_groups=groups
        )

    if tiled:
        flat = spectra.reshape(channels, 2, length // LANES, LANES).transpose(0, 2, 1, 3)
        flat = flat.reshape(-1, LANES)
        sent = pl.pallas_call(
            functools.partial(prep_kernel, order, blocks),
            out_shape=jax.ShapeDtypeStruct((count, rows_in, LANES), f32),
            in_specs=[vmem],
            out_specs=vmem,
        )(flat)
        received = exchange(sent)
        inner = order
    else:
        cut = spectra.reshape(sub, 4, 2, count, blocks, LANES).transpose(3, 1, 4, 2, 0, 5)
        tail = spectra.reshape(sub, 4, 2, count, frames)[..., frames - HALO :]
        tail = jnp.concatenate([jnp.zeros_like(tail[..., :1, :]), tail[..., :-1, :]], axis=3)
        tail = tail.transpose(3, 2, 0, 1, 4).reshape(count, 2 * sub, LANES)
        sent = jnp.concatenate([cut.reshape(count, 8 * blocks * sub, LANES), tail], axis=1)
        received = exchange(sent[np.array(order)])
        received = received[np.argsort(np.array(order))]
        tiles = 8 * blocks + 2
        inner = tuple(range(width // 4 // SUB))
        received = received.reshape(count, tiles, sub, LANES).transpose(1, 0, 2, 3)
        received = received.reshape(tiles, len(inner), SUB, LANES).transpose(1, 0, 2, 3)
        received = received.reshape(len(inner), tiles * SUB, LANES)

    w_hi, w_lo = radix4_tables(width)
    res = resampler_tables()
    rows = ((frames + HALO) // 4 - 4 + SUB) // SUB * SUB
    made = pl.pallas_call(
        functools.partial(main_kernel, inner, frames),
        out_shape=jax.ShapeDtypeStruct((len(inner), rows_out, LANES), f32),
        in_specs=[vmem] * 6,
        out_specs=vmem,
        scratch_shapes=[
            pltpu.VMEM((4, frames + HALO, 2 * LANES), f32),
            pltpu.VMEM((8, frames + HALO + 16, LANES), f32),
            pltpu.VMEM((32, rows + SUB, LANES), f32),
            pltpu.VMEM((4, 10 * rows, LANES), bf16),
            pltpu.VMEM((4, 10 * rows, LANES), bf16),
            pltpu.VMEM((40, rows, LANES), f32),
            pltpu.VMEM((8, outs, LANES), f32),
            pltpu.VMEM((4, outs + outs % LANES, 2 * LANES), bf16),
            pltpu.VMEM((4, outs + outs % LANES, 2 * LANES), bf16),
        ],
    )(received, w_hi, w_lo, res, synth_taps, analysis_taps)

    if tiled:
        back = exchange(made)
        out = pl.pallas_call(
            functools.partial(final_kernel, order),
            out_shape=jax.ShapeDtypeStruct((channels * 2 * count * outs // LANES, LANES), f32),
            in_specs=[vmem],
            out_specs=vmem,
        )(back)
        out = out.reshape(channels, count * outs // LANES, 2, LANES).transpose(0, 2, 1, 3)
        return out.reshape(channels, 2, count * outs)
    tiles = rows_out // SUB
    made = made.reshape(len(inner), tiles, SUB, LANES).transpose(1, 0, 2, 3)
    made = made.reshape(tiles, count, sub, LANES).transpose(1, 0, 2, 3)
    back = exchange(made[np.array(order)])
    back = back[np.argsort(np.array(order))]
    full = outs // LANES
    head = back[:, : 8 * full].reshape(count, full, 4, 2, sub, LANES).transpose(4, 2, 3, 0, 1, 5)
    head = head.reshape(channels, 2, count, full * LANES)
    rest = back[:, 8 * full :].reshape(count, 4, sub, 2, outs - full * LANES).transpose(2, 1, 3, 0, 4)
    rest = rest.reshape(channels, 2, count, -1)
    return jnp.concatenate([head, rest], axis=3).reshape(channels, 2, count * outs)


def solution(mesh):
    in_specs = (P("tm", "station", None), P(), P())
    out_specs = P("tm", "station", None)
    order = list(range(mesh.shape["tm"]))[::-1]
    return jax.shard_map(
        functools.partial(shards, order),
        mesh=mesh,
        in_specs=in_specs,
        out_specs=out_specs,
        check_vma=False,
    )
```

```python
import functools
import math

import jax
import jax.numpy as jnp
import numpy as np
from jax import lax
from jax.experimental import pallas as pl
from jax.experimental.pallas import tpu as pltpu
from jax.sharding import PartitionSpec as P

RT = 32
PHASES = 64
UP, DOWN = 5, 4
LANES = 128
SUB = 8
ORDER = [5, 2, 7, 13, 12, 11, 0, 4, 8, 15, 6, 14, 10, 3, 9, 1]
HALO = 32


def split(value):
    high = value.astype(jnp.bfloat16)
    low = (value - high.astype(jnp.float32)).astype(jnp.bfloat16)
    return high, low


def np_split(value):
    value = value.astype(np.float32)
    high = value.astype(jnp.bfloat16)
    low = (value - high.astype(np.float32)).astype(jnp.bfloat16)
    return high, low


def radix4_tables(width):
    quarter = width // 4
    k = np.arange(quarter)[:, None]
    m = np.arange(quarter)[None, :]
    blocks = []
    for r in range(4):
        angle = ((4 * k + r) * m % width) * (2.0 * math.pi / width)
        cosine = np.cos(angle) / math.sqrt(width)
        sine = np.sin(angle) / math.sqrt(width)
        blocks.append(np.block([[cosine, sine], [-sine, cosine]]))
    return np_split(np.stack(blocks))


def resampler_tables():
    parts = []
    for j in range(UP):
        sample = np.arange(LANES)[None, :] + LANES * j
        start = 128 * (min(j, 3) - 1)
        column = np.arange(2 * LANES)[:, None] + start
        lag = DOWN * sample // UP - column
        phase = PHASES * (DOWN * sample % UP) // UP
        offset = lag + phase / PHASES - (RT // 2 - 1)
        window = 0.5 + 0.5 * np.cos(math.pi * offset / (RT / 2.0))
        coeff = 0.9 * np.sinc(0.9 * offset) * window
        parts.append(np_split(np.where((lag >= 0) & (lag < RT), coeff, 0.0)))
    out = [np.concatenate([high, low], axis=1) for high, low in parts[:3]]
    out.append(np.concatenate([parts[3][0], parts[4][0]], axis=1))
    out.append(np.concatenate([parts[3][1], parts[4][1]], axis=1))
    return np.stack(out)


def lane_iota():
    return lax.broadcasted_iota(jnp.int32, (SUB, LANES), 1)


def prep_kernel(order, blocks, x_ref, o_ref):
    stride = x_ref.shape[0] // (4 * SUB)
    lane = lane_iota()

    def tile(r, k, part):
        return x_ref[pl.ds(r * stride + 2 * k + part, SUB, stride=4 * stride), :]

    for place, dev in enumerate(order):
        for r in range(4):
            for lb in range(blocks):
                for part in range(2):
                    t = (r * blocks + lb) * 2 + part
                    o_ref[place, t * SUB : (t + 1) * SUB, :] = tile(r, blocks * dev + lb, part)
        for part in range(2):
            total = jnp.zeros((SUB, LANES), jnp.float32)
            if dev > 0:
                for r in range(4):
                    value = tile(r, blocks * dev - 1, part)
                    if r < 3:
                        value = pltpu.roll(value, HALO * (r + 1), 1)
                    total = jnp.where(lane // HALO == r, value, total)
            t = 8 * blocks + part
            o_ref[place, t * SUB : (t + 1) * SUB, :] = total


def main_kernel(
    order, frames, x_ref, w_hi, w_lo, res_ref, st_ref, at_ref, o_ref,
    a_ref, v_ref, y_ref, yh_ref, yl_ref, z_ref, u_ref, bh_ref, bl_ref,
):
    blocks = frames // LANES
    count = len(order)
    place_of = {dev: place for place, dev in enumerate(order)}
    f32 = jnp.float32

    def dot(a, b):
        return lax.dot_general(a, b, (((1,), (0,)), ((), ())), preferred_element_type=f32)

    def dot_t(a, b):
        return lax.dot_general(a, b, (((1,), (1,)), ((), ())), preferred_element_type=f32)

    def tile(t):
        return jnp.concatenate(
            [x_ref[place_of[s], t * SUB : (t + 1) * SUB, :] for s in range(count)], axis=0
        )

    halo = [tile(8 * blocks + part).T for part in range(2)]
    for r in range(4):
        rows = [jnp.concatenate([h[r * HALO : (r + 1) * HALO] for h in halo], axis=1)]
        for lb in range(blocks):
            rows.append(
                jnp.concatenate([tile((r * blocks + lb) * 2 + part).T for part in range(2)], axis=1)
            )
        high, low = split(jnp.concatenate(rows, axis=0))
        a_ref[r] = dot(high, w_hi[r]) + dot(low, w_hi[r]) + dot(high, w_lo[r])

    total = frames + HALO

    @pl.loop(0, total // 16)
    def _(i):
        row = pl.ds(pl.multiple_of(i * 16, 16), 16)
        re = [a_ref[r, row, :LANES] for r in range(4)]
        im = [a_ref[r, row, LANES:] for r in range(4)]
        sr, dr = re[0] + re[2], re[0] - re[2]
        si, di = im[0] + im[2], im[0] - im[2]
        tr, er = re[1] + re[3], re[1] - re[3]
        ti, ei = im[1] + im[3], im[1] - im[3]
        v_ref[0, row, :] = sr + tr
        v_ref[4, row, :] = si + ti
        v_ref[1, row, :] = dr - ei
        v_ref[5, row, :] = di + er
        v_ref[2, row, :] = sr - tr
        v_ref[6, row, :] = si - ti
        v_ref[3, row, :] = dr + ei
        v_ref[7, row, :] = di - er

    for k in range(8):
        v_ref[k, total : total + 16, :] = jnp.zeros((16, LANES), f32)
        y_ref[k * 2, 0:SUB, :] = jnp.zeros((SUB, LANES), f32)
        y_ref[k * 2 + 1, 0:SUB, :] = jnp.zeros((SUB, LANES), f32)
        y_ref[16 + k * 2, 0:SUB, :] = jnp.zeros((SUB, LANES), f32)
        y_ref[16 + k * 2 + 1, 0:SUB, :] = jnp.zeros((SUB, LANES), f32)

    taps_len = st_ref.shape[0]
    groups = (total // 4 - 4 + SUB) // SUB
    for q in range(4):

        @pl.loop(0, groups)
        def _(t):
            base = t * 32 + 16
            accs = {}
            vals = {}

            def load(part, j):
                vals[part, j] = v_ref[part * 4 + q, pl.ds(base + j, SUB, stride=4), :]

            for part in range(2):
                for j in range(1, 4):
                    load(part, j)
            for p in range(taps_len):
                tap = jnp.broadcast_to(
                    st_ref[p : p + 1, q * LANES : (q + 1) * LANES], (SUB, LANES)
                )
                for part in range(2):
                    load(part, -p)
                    for b in range(4):
                        term = tap * vals[part, b - p]
                        accs[part, b] = term if p == 0 else accs[part, b] + term
            for part in range(2):
                for b in range(4):
                    row = pl.ds(pl.multiple_of(t * SUB, SUB) + SUB, SUB)
                    y_ref[part * 16 + b * 4 + q, row, :] = accs[part, b]

    rows = groups * SUB
    both = 2 * rows
    for b in range(4):
        for q in range(4):
            value = jnp.concatenate(
                [y_ref[part * 16 + b * 4 + q, SUB : SUB + rows, :] for part in range(2)], axis=0
            )
            high, low = split(value)
            first = b * both + (both if q == 3 else 0)
            yh_ref[q, first : first + both, :] = high
            yl_ref[q, first : first + both, :] = low
    value = jnp.concatenate(
        [y_ref[part * 16 + 15, SUB - 1 : SUB - 1 + rows, :] for part in range(2)], axis=0
    )
    high, low = split(value)
    yh_ref[3, 0:both, :] = high
    yl_ref[3, 0:both, :] = low

    def store_z(j, value):
        for b in range(4):
            g, q = (5 * b + j) // 4, (5 * b + j) % 4
            for part in range(2):
                first = b * both + part * rows
                z_ref[part * 20 + g * 4 + q] = value[first : first + rows]

    def pair(ref, left, right):
        first = both if left == 2 else 0
        a = ref[3, 0 : 4 * both] if left < 0 else ref[left, 0 : 4 * both]
        return jnp.concatenate([a, ref[right, first if right == 3 else 0 : (first if right == 3 else 0) + 4 * both]], axis=1)

    for j in range(3):
        high = pair(yh_ref, j - 1, j)
        low = pair(yl_ref, j - 1, j)
        wide = dot(high, res_ref[j])
        store_z(j, wide[:, :LANES] + wide[:, LANES:] + dot(low, res_ref[j, :, :LANES]))
    high = pair(yh_ref, 2, 3)
    low = pair(yl_ref, 2, 3)
    wide = dot(high, res_ref[3]) + dot(high, res_ref[4]) + dot(low, res_ref[3])
    store_z(3, wide[:, :LANES])
    store_z(4, wide[:, LANES:])

    outs = frames * UP // DOWN
    taps_len = at_ref.shape[0]
    groups2 = frames // 4 // SUB
    for q in range(4):

        @pl.loop(0, groups2)
        def _(t):
            accs = {}
            vals = {}

            def load(part, j):
                shift = j // UP
                slot = part * 20 + (j - UP * shift) * 4 + q
                vals[part, j] = z_ref[slot, pl.ds(t * SUB + 4 + shift, SUB), :]

            for part in range(2):
                for j in range(1, UP):
                    load(part, j)
            for p in range(taps_len):
                tap = jnp.broadcast_to(
                    at_ref[p : p + 1, q * LANES : (q + 1) * LANES], (SUB, LANES)
                )
                for part in range(2):
                    load(part, -p)
                    for g in range(UP):
                        term = tap * vals[part, g - p]
                        accs[part, g] = term if p == 0 else accs[part, g] + term
            for part in range(2):
                for g in range(UP):
                    row = pl.ds(t * SUB * UP + g, SUB, stride=UP)
                    u_ref[part * 4 + q, row, :] = accs[part, g]

    @pl.loop(0, outs // 16)
    def _(i):
        row = pl.ds(pl.multiple_of(i * 16, 16), 16)
        re = [u_ref[q, row, :] for q in range(4)]
        im = [u_ref[4 + q, row, :] for q in range(4)]
        sr, dr = re[0] + re[2], re[0] - re[2]
        si, di = im[0] + im[2], im[0] - im[2]
        tr, er = re[1] + re[3], re[1] - re[3]
        ti, ei = im[1] + im[3], im[1] - im[3]
        spectra = [
            (sr + tr, si + ti), (dr + ei, di - er), (sr - tr, si - ti), (dr - ei, di + er)
        ]
        for r in range(4):
            for part in range(2):
                high, low = split(spectra[r][part])
                cols = slice(part * LANES, (part + 1) * LANES)
                bh_ref[r, row, cols] = high
                bl_ref[r, row, cols] = low

    lane = lax.broadcasted_iota(jnp.int32, (LANES, LANES), 1)
    full = outs // LANES
    rest = outs - full * LANES
    for r in range(4):
        for place in range(2):
            first = full * LANES + place * rest
            last = slice(full * LANES, full * LANES + rest)
            if place == 1:
                bh_ref[r, first : first + rest] = bh_ref[r, last]
            bh_ref[r, first + LANES : first + LANES + rest] = bl_ref[r, last]
        main = slice(0, full * LANES)
        high, low = bh_ref[r, main], bl_ref[r, main]
        out = dot_t(w_hi[r], high) + dot_t(w_hi[r], low) + dot_t(w_lo[r], high)
        tail = dot_t(w_hi[r], bh_ref[r, full * LANES :])
        tail = tail[:, :LANES] + tail[:, LANES:]
        tail = tail + dot_t(w_lo[r], bh_ref[r, full * LANES : (full + 1) * LANES])
        for part in range(2):
            for k in range(full):
                t = k * SUB + r * 2 + part
                value = out[part * LANES : (part + 1) * LANES, k * LANES : (k + 1) * LANES]
                for place, dev in enumerate(order):
                    o_ref[place, t * SUB : (t + 1) * SUB, :] = value[dev * SUB : (dev + 1) * SUB]
        value = jnp.where(lane < rest, tail[:LANES], tail[LANES:])
        t = full * SUB + r
        for place, dev in enumerate(order):
            o_ref[place, t * SUB : (t + 1) * SUB, :] = value[dev * SUB : (dev + 1) * SUB]


def final_kernel(order, x_ref, o_ref):
    stride = o_ref.shape[0] // (4 * SUB)
    lane = lane_iota()
    half = LANES // 2
    place_of = {dev: place for place, dev in enumerate(order)}

    def tile(dev, t):
        return x_ref[place_of[dev], t * SUB : (t + 1) * SUB, :]

    for dev in range(0, len(order), 2):
        for r in range(4):
            for part in range(2):
                t = r * 2 + part
                ends = [tile(dev, 16 + r), tile(dev + 1, 16 + r)]
                ends[1 - part] = pltpu.roll(ends[1 - part], half, 1)
                r0 = pltpu.roll(tile(dev + 1, t), half, 1)
                r1 = pltpu.roll(tile(dev + 1, 8 + t), half, 1)
                values = [
                    tile(dev, t),
                    tile(dev, 8 + t),
                    jnp.where(lane < half, ends[0], r0),
                    jnp.where(lane < half, r0, r1),
                    jnp.where(lane < half, r1, ends[1]),
                ]
                for k, value in enumerate(values):
                    first = r * stride + (5 * (dev // 2) + k) * 2 + part
                    o_ref[pl.ds(first, SUB, stride=4 * stride), :] = value


def shards(order, spectra, synth_taps, analysis_taps):
    count = lax.axis_size("tm")
    channels, parts, length = spectra.shape
    width = channels * count
    frames = length // count
    outs = frames * UP // DOWN
    blocks = frames // LANES
    order = tuple(order)
    groups = [list(order)]
    tiled = channels == 4 * SUB
    vmem = pl.BlockSpec(memory_space=pltpu.VMEM)
    f32, bf16 = jnp.float32, jnp.bfloat16
    rows_in = 8 * blocks * SUB + 2 * SUB
    rows_out = (outs * 64) // LANES
    sub = channels // 4
    small = pltpu.CompilerParams(vmem_limit_bytes=8 << 20)

    def exchange(value):
        return lax.all_to_all(
            value, "tm", split_axis=0, concat_axis=0, tiled=True, axis_index_groups=groups
        )

    if tiled:
        flat = spectra.reshape(channels, 2, length // LANES, LANES).transpose(0, 2, 1, 3)
        flat = flat.reshape(-1, LANES)
        sent = pl.pallas_call(
            functools.partial(prep_kernel, order, blocks),
            out_shape=jax.ShapeDtypeStruct((count, rows_in, LANES), f32),
            in_specs=[vmem],
            out_specs=vmem,
            compiler_params=small,
        )(flat)
        received = exchange(sent)
        inner = order
    else:
        cut = spectra.reshape(sub, 4, 2, count, blocks, LANES).transpose(3, 1, 4, 2, 0, 5)
        tail = spectra.reshape(sub, 4, 2, count, frames)[..., frames - HALO :]
        tail = jnp.concatenate([jnp.zeros_like(tail[..., :1, :]), tail[..., :-1, :]], axis=3)
        tail = tail.transpose(3, 2, 0, 1, 4).reshape(count, 2 * sub, LANES)
        sent = jnp.concatenate([cut.reshape(count, 8 * blocks * sub, LANES), tail], axis=1)
        received = exchange(sent[np.array(order)])
        received = received[np.argsort(np.array(order))]
        tiles = 8 * blocks + 2
        inner = tuple(range(width // 4 // SUB))
        received = received.reshape(count, tiles, sub, LANES).transpose(1, 0, 2, 3)
        received = received.reshape(tiles, len(inner), SUB, LANES).transpose(1, 0, 2, 3)
        received = received.reshape(len(inner), tiles * SUB, LANES)

    w_hi, w_lo = radix4_tables(width)
    res = resampler_tables()
    rows = ((frames + HALO) // 4 - 4 + SUB) // SUB * SUB
    made = pl.pallas_call(
        functools.partial(main_kernel, inner, frames),
        out_shape=jax.ShapeDtypeStruct((len(inner), rows_out, LANES), f32),
        in_specs=[vmem] * 6,
        out_specs=vmem,
        scratch_shapes=[
            pltpu.VMEM((4, frames + HALO, 2 * LANES), f32),
            pltpu.VMEM((8, frames + HALO + 16, LANES), f32),
            pltpu.VMEM((32, rows + SUB, LANES), f32),
            pltpu.VMEM((4, 10 * rows, LANES), bf16),
            pltpu.VMEM((4, 10 * rows, LANES), bf16),
            pltpu.VMEM((40, rows, LANES), f32),
            pltpu.VMEM((8, outs, LANES), f32),
            pltpu.VMEM((4, outs + 3 * (outs % LANES), 2 * LANES), bf16),
            pltpu.VMEM((4, outs, 2 * LANES), bf16),
        ],
        compiler_params=pltpu.CompilerParams(vmem_limit_bytes=24 << 20),
    )(received, w_hi, w_lo, res, synth_taps, analysis_taps)

    if tiled:
        back = exchange(made)
        out = pl.pallas_call(
            functools.partial(final_kernel, order),
            out_shape=jax.ShapeDtypeStruct((channels * 2 * count * outs // LANES, LANES), f32),
            in_specs=[vmem],
            out_specs=vmem,
            compiler_params=small,
        )(back)
        out = out.reshape(channels, count * outs // LANES, 2, LANES).transpose(0, 2, 1, 3)
        return out.reshape(channels, 2, count * outs)
    tiles = rows_out // SUB
    made = made.reshape(len(inner), tiles, SUB, LANES).transpose(1, 0, 2, 3)
    made = made.reshape(tiles, count, sub, LANES).transpose(1, 0, 2, 3)
    back = exchange(made[np.array(order)])
    back = back[np.argsort(np.array(order))]
    full = outs // LANES
    head = back[:, : 8 * full].reshape(count, full, 4, 2, sub, LANES).transpose(4, 2, 3, 0, 1, 5)
    head = head.reshape(channels, 2, count, full * LANES)
    rest = back[:, 8 * full :].reshape(count, 4, sub, 2, outs - full * LANES).transpose(2, 1, 3, 0, 4)
    rest = rest.reshape(channels, 2, count, -1)
    return jnp.concatenate([head, rest], axis=3).reshape(channels, 2, count * outs)


def solution(mesh):
    in_specs = (P("tm", "station", None), P(), P())
    out_specs = P("tm", "station", None)
    order = list(range(mesh.shape["tm"]))
    if len(order) == len(ORDER):
        order = ORDER
    return jax.shard_map(
        functools.partial(shards, order),
        mesh=mesh,
        in_specs=in_specs,
        out_specs=out_specs,
        check_vma=False,
    )
```

```python
import functools
import math

import jax
import jax.numpy as jnp
import numpy as np
from jax import lax
from jax.experimental import pallas as pl
from jax.experimental.pallas import tpu as pltpu
from jax.sharding import PartitionSpec as P

RT = 32
PHASES = 64
UP, DOWN = 5, 4
LANES = 128
SUB = 8
ORDER = [5, 2, 7, 13, 12, 11, 0, 4, 8, 15, 6, 14, 10, 3, 9, 1]
PREP_VMEM = 8 << 20
HALO = 32


def split(value):
    high = value.astype(jnp.bfloat16)
    low = (value - high.astype(jnp.float32)).astype(jnp.bfloat16)
    return high, low


def np_split(value):
    value = value.astype(np.float32)
    high = value.astype(jnp.bfloat16)
    low = (value - high.astype(np.float32)).astype(jnp.bfloat16)
    return high, low


def radix4_tables(width):
    quarter = width // 4
    k = np.arange(quarter)[:, None]
    m = np.arange(quarter)[None, :]
    blocks = []
    for r in range(4):
        angle = ((4 * k + r) * m % width) * (2.0 * math.pi / width)
        cosine = np.cos(angle) / math.sqrt(width)
        sine = np.sin(angle) / math.sqrt(width)
        blocks.append(np.block([[cosine, sine], [-sine, cosine]]))
    return np_split(np.stack(blocks))


def resampler_tables():
    parts = []
    for j in range(UP):
        sample = np.arange(LANES)[None, :] + LANES * j
        start = 128 * (min(j, 3) - 1)
        column = np.arange(2 * LANES)[:, None] + start
        lag = DOWN * sample // UP - column
        phase = PHASES * (DOWN * sample % UP) // UP
        offset = lag + phase / PHASES - (RT // 2 - 1)
        window = 0.5 + 0.5 * np.cos(math.pi * offset / (RT / 2.0))
        coeff = 0.9 * np.sinc(0.9 * offset) * window
        parts.append(np_split(np.where((lag >= 0) & (lag < RT), coeff, 0.0)))
    out = [np.concatenate([high, low], axis=1) for high, low in parts[:3]]
    out.append(np.concatenate([parts[3][0], parts[4][0]], axis=1))
    out.append(np.concatenate([parts[3][1], parts[4][1]], axis=1))
    return np.stack(out)


def lane_iota():
    return lax.broadcasted_iota(jnp.int32, (SUB, LANES), 1)


def prep_kernel(order, blocks, x_ref, o_ref, buf_ref, sems):
    sub, _, length, _ = x_ref.shape
    lane = lane_iota()
    copies = [
        pltpu.make_async_copy(x_ref.at[:, r], buf_ref.at[r], sems.at[r]) for r in range(4)
    ]
    for copy in copies:
        copy.start()
    for r in range(4):
        copies[r].wait()
        flat_ref = buf_ref.at[r].reshape(sub * length, LANES)
        for place, dev in enumerate(order):
            for lb in range(blocks):
                for part in range(2):
                    t = (r * blocks + lb) * 2 + part
                    row = 2 * (blocks * dev + lb) + part
                    o_ref[place, t * SUB : (t + 1) * SUB, :] = flat_ref[
                        pl.ds(row, SUB, stride=length), :
                    ]
    for place, dev in enumerate(order):
        for part in range(2):
            total = jnp.zeros((SUB, LANES), jnp.float32)
            if dev > 0:
                last = order.index(dev - 1)
                for r in range(4):
                    t = (r * blocks + blocks - 1) * 2 + part
                    value = o_ref[last, t * SUB : (t + 1) * SUB, :]
                    if r < 3:
                        value = pltpu.roll(value, HALO * (r + 1), 1)
                    total = jnp.where(lane // HALO == r, value, total)
            t = 8 * blocks + part
            o_ref[place, t * SUB : (t + 1) * SUB, :] = total


def main_kernel(
    order, frames, x_ref, w_hi, w_lo, res_ref, st_ref, at_ref, o_ref,
    a_ref, v_ref, y_ref, yh_ref, yl_ref, z_ref, u_ref, bh_ref, bl_ref,
):
    blocks = frames // LANES
    count = len(order)
    place_of = {dev: place for place, dev in enumerate(order)}
    f32 = jnp.float32

    def dot(a, b):
        return lax.dot_general(a, b, (((1,), (0,)), ((), ())), preferred_element_type=f32)

    def dot_t(a, b):
        return lax.dot_general(a, b, (((1,), (1,)), ((), ())), preferred_element_type=f32)

    def tile(t):
        return jnp.concatenate(
            [x_ref[place_of[s], t * SUB : (t + 1) * SUB, :] for s in range(count)], axis=0
        )

    halo = [tile(8 * blocks + part).T for part in range(2)]
    for r in range(4):
        rows = [jnp.concatenate([h[r * HALO : (r + 1) * HALO] for h in halo], axis=1)]
        for lb in range(blocks):
            rows.append(
                jnp.concatenate([tile((r * blocks + lb) * 2 + part).T for part in range(2)], axis=1)
            )
        high, low = split(jnp.concatenate(rows, axis=0))
        a_ref[r] = dot(high, w_hi[r]) + dot(low, w_hi[r]) + dot(high, w_lo[r])

    total = frames + HALO

    @pl.loop(0, total // 16)
    def _(i):
        row = pl.ds(pl.multiple_of(i * 16, 16), 16)
        re = [a_ref[r, row, :LANES] for r in range(4)]
        im = [a_ref[r, row, LANES:] for r in range(4)]
        sr, dr = re[0] + re[2], re[0] - re[2]
        si, di = im[0] + im[2], im[0] - im[2]
        tr, er = re[1] + re[3], re[1] - re[3]
        ti, ei = im[1] + im[3], im[1] - im[3]
        v_ref[0, row, :] = sr + tr
        v_ref[4, row, :] = si + ti
        v_ref[1, row, :] = dr - ei
        v_ref[5, row, :] = di + er
        v_ref[2, row, :] = sr - tr
        v_ref[6, row, :] = si - ti
        v_ref[3, row, :] = dr + ei
        v_ref[7, row, :] = di - er

    for k in range(8):
        v_ref[k, total : total + 16, :] = jnp.zeros((16, LANES), f32)
        y_ref[k * 2, 0:SUB, :] = jnp.zeros((SUB, LANES), f32)
        y_ref[k * 2 + 1, 0:SUB, :] = jnp.zeros((SUB, LANES), f32)
        y_ref[16 + k * 2, 0:SUB, :] = jnp.zeros((SUB, LANES), f32)
        y_ref[16 + k * 2 + 1, 0:SUB, :] = jnp.zeros((SUB, LANES), f32)

    taps_len = st_ref.shape[0]
    groups = (total // 4 - 4 + SUB) // SUB
    for q in range(4):

        @pl.loop(0, groups, unroll=3)
        def _(t):
            base = t * 32 + 16
            accs = {}
            vals = {}

            def load(part, j):
                vals[part, j] = v_ref[part * 4 + q, pl.ds(base + j, SUB, stride=4), :]

            for part in range(2):
                for j in range(1, 4):
                    load(part, j)
            for p in range(taps_len):
                tap = jnp.broadcast_to(
                    st_ref[p : p + 1, q * LANES : (q + 1) * LANES], (SUB, LANES)
                )
                for part in range(2):
                    load(part, -p)
                    for b in range(4):
                        term = tap * vals[part, b - p]
                        accs[part, b] = term if p == 0 else accs[part, b] + term
            for part in range(2):
                for b in range(4):
                    row = pl.ds(pl.multiple_of(t * SUB, SUB) + SUB, SUB)
                    y_ref[part * 16 + b * 4 + q, row, :] = accs[part, b]

    rows = groups * SUB
    both = 2 * rows
    for b in range(4):
        for q in range(4):
            value = jnp.concatenate(
                [y_ref[part * 16 + b * 4 + q, SUB : SUB + rows, :] for part in range(2)], axis=0
            )
            high, low = split(value)
            first = b * both + (both if q == 3 else 0)
            yh_ref[q, first : first + both, :] = high
            yl_ref[q, first : first + both, :] = low
    value = jnp.concatenate(
        [y_ref[part * 16 + 15, SUB - 1 : SUB - 1 + rows, :] for part in range(2)], axis=0
    )
    high, low = split(value)
    yh_ref[3, 0:both, :] = high
    yl_ref[3, 0:both, :] = low

    def store_z(j, value):
        for b in range(4):
            g, q = (5 * b + j) // 4, (5 * b + j) % 4
            for part in range(2):
                first = b * both + part * rows
                z_ref[part * 20 + g * 4 + q] = value[first : first + rows]

    def pair(ref, left, right):
        first = both if left == 2 else 0
        a = ref[3, 0 : 4 * both] if left < 0 else ref[left, 0 : 4 * both]
        return jnp.concatenate([a, ref[right, first if right == 3 else 0 : (first if right == 3 else 0) + 4 * both]], axis=1)

    for j in range(3):
        high = pair(yh_ref, j - 1, j)
        low = pair(yl_ref, j - 1, j)
        wide = dot(high, res_ref[j])
        store_z(j, wide[:, :LANES] + wide[:, LANES:] + dot(low, res_ref[j, :, :LANES]))
    high = pair(yh_ref, 2, 3)
    low = pair(yl_ref, 2, 3)
    wide = dot(high, res_ref[3]) + dot(high, res_ref[4]) + dot(low, res_ref[3])
    store_z(3, wide[:, :LANES])
    store_z(4, wide[:, LANES:])

    outs = frames * UP // DOWN
    taps_len = at_ref.shape[0]
    groups2 = frames // 4 // SUB
    for q in range(4):

        @pl.loop(0, groups2, unroll=2)
        def _(t):
            accs = {}
            vals = {}

            def load(part, j):
                shift = j // UP
                slot = part * 20 + (j - UP * shift) * 4 + q
                vals[part, j] = z_ref[slot, pl.ds(t * SUB + 4 + shift, SUB), :]

            for part in range(2):
                for j in range(1, UP):
                    load(part, j)
            for p in range(taps_len):
                tap = jnp.broadcast_to(
                    at_ref[p : p + 1, q * LANES : (q + 1) * LANES], (SUB, LANES)
                )
                for part in range(2):
                    load(part, -p)
                    for g in range(UP):
                        term = tap * vals[part, g - p]
                        accs[part, g] = term if p == 0 else accs[part, g] + term
            for part in range(2):
                for g in range(UP):
                    row = pl.ds(t * SUB * UP + g, SUB, stride=UP)
                    u_ref[part * 4 + q, row, :] = accs[part, g]

    @pl.loop(0, outs // 16)
    def _(i):
        row = pl.ds(pl.multiple_of(i * 16, 16), 16)
        re = [u_ref[q, row, :] for q in range(4)]
        im = [u_ref[4 + q, row, :] for q in range(4)]
        sr, dr = re[0] + re[2], re[0] - re[2]
        si, di = im[0] + im[2], im[0] - im[2]
        tr, er = re[1] + re[3], re[1] - re[3]
        ti, ei = im[1] + im[3], im[1] - im[3]
        spectra = [
            (sr + tr, si + ti), (dr + ei, di - er), (sr - tr, si - ti), (dr - ei, di + er)
        ]
        for r in range(4):
            for part in range(2):
                high, low = split(spectra[r][part])
                cols = slice(part * LANES, (part + 1) * LANES)
                bh_ref[r, row, cols] = high
                bl_ref[r, row, cols] = low

    lane = lax.broadcasted_iota(jnp.int32, (LANES, LANES), 1)
    full = outs // LANES
    rest = outs - full * LANES
    for r in range(4):
        for place in range(2):
            first = full * LANES + place * rest
            last = slice(full * LANES, full * LANES + rest)
            if place == 1:
                bh_ref[r, first : first + rest] = bh_ref[r, last]
            bh_ref[r, first + LANES : first + LANES + rest] = bl_ref[r, last]
        main = slice(0, full * LANES)
        high, low = bh_ref[r, main], bl_ref[r, main]
        out = dot_t(w_hi[r], high) + dot_t(w_hi[r], low) + dot_t(w_lo[r], high)
        tail = dot_t(w_hi[r], bh_ref[r, full * LANES :])
        tail = tail[:, :LANES] + tail[:, LANES:]
        tail = tail + dot_t(w_lo[r], bh_ref[r, full * LANES : (full + 1) * LANES])
        for part in range(2):
            for k in range(full):
                t = k * SUB + r * 2 + part
                value = out[part * LANES : (part + 1) * LANES, k * LANES : (k + 1) * LANES]
                for place, dev in enumerate(order):
                    o_ref[place, t * SUB : (t + 1) * SUB, :] = value[dev * SUB : (dev + 1) * SUB]
        value = jnp.where(lane < rest, tail[:LANES], tail[LANES:])
        t = full * SUB + r
        for place, dev in enumerate(order):
            o_ref[place, t * SUB : (t + 1) * SUB, :] = value[dev * SUB : (dev + 1) * SUB]


def final_kernel(order, x_ref, o_ref, buf_ref, sems):
    _, _, length, _ = o_ref.shape
    lane = lane_iota()
    half = LANES // 2
    place_of = {dev: place for place, dev in enumerate(order)}
    copies = []

    def tile(dev, t):
        return x_ref[place_of[dev], t * SUB : (t + 1) * SUB, :]

    for r in range(4):
        flat_ref = buf_ref.at[r].reshape(SUB * length, LANES)
        for dev in range(0, len(order), 2):
            for part in range(2):
                t = r * 2 + part
                ends = [tile(dev, 16 + r), tile(dev + 1, 16 + r)]
                ends[1 - part] = pltpu.roll(ends[1 - part], half, 1)
                r0 = pltpu.roll(tile(dev + 1, t), half, 1)
                r1 = pltpu.roll(tile(dev + 1, 8 + t), half, 1)
                values = [
                    tile(dev, t),
                    tile(dev, 8 + t),
                    jnp.where(lane < half, ends[0], r0),
                    jnp.where(lane < half, r0, r1),
                    jnp.where(lane < half, r1, ends[1]),
                ]
                for k, value in enumerate(values):
                    first = (5 * (dev // 2) + k) * 2 + part
                    flat_ref[pl.ds(first, SUB, stride=length), :] = value
        copies.append(pltpu.make_async_copy(buf_ref.at[r], o_ref.at[:, r], sems.at[r]))
        copies[-1].start()
    for copy in copies:
        copy.wait()


def shards(order, spectra, synth_taps, analysis_taps):
    count = lax.axis_size("tm")
    channels, parts, length = spectra.shape
    width = channels * count
    frames = length // count
    outs = frames * UP // DOWN
    blocks = frames // LANES
    order = tuple(order)
    groups = [list(order)]
    tiled = channels == 4 * SUB
    vmem = pl.BlockSpec(memory_space=pltpu.VMEM)
    hbm = pl.BlockSpec(memory_space=pltpu.HBM)
    f32, bf16 = jnp.float32, jnp.bfloat16
    rows_in = 8 * blocks * SUB + 2 * SUB
    rows_out = (outs * 64) // LANES
    sub = channels // 4
    small = pltpu.CompilerParams(vmem_limit_bytes=8 << 20)

    def exchange(value):
        return lax.all_to_all(
            value, "tm", split_axis=0, concat_axis=0, tiled=True, axis_index_groups=groups
        )

    if tiled:
        flat = spectra.reshape(channels, 2, length // LANES, LANES).transpose(0, 2, 1, 3)
        flat = flat.reshape(sub, 4, -1, LANES)
        flat = pltpu.with_memory_space_constraint(flat, pltpu.HBM)
        sent = pl.pallas_call(
            functools.partial(prep_kernel, order, blocks),
            out_shape=jax.ShapeDtypeStruct((count, rows_in, LANES), f32),
            in_specs=[hbm],
            out_specs=vmem,
            scratch_shapes=[
                pltpu.VMEM((4, sub) + flat.shape[2:], f32),
                pltpu.SemaphoreType.DMA((4,)),
            ],
            compiler_params=pltpu.CompilerParams(vmem_limit_bytes=PREP_VMEM),
        )(flat)
        received = exchange(sent)
        inner = order
    else:
        cut = spectra.reshape(sub, 4, 2, count, blocks, LANES).transpose(3, 1, 4, 2, 0, 5)
        tail = spectra.reshape(sub, 4, 2, count, frames)[..., frames - HALO :]
        tail = jnp.concatenate([jnp.zeros_like(tail[..., :1, :]), tail[..., :-1, :]], axis=3)
        tail = tail.transpose(3, 2, 0, 1, 4).reshape(count, 2 * sub, LANES)
        sent = jnp.concatenate([cut.reshape(count, 8 * blocks * sub, LANES), tail], axis=1)
        received = exchange(sent[np.array(order)])
        received = received[np.argsort(np.array(order))]
        tiles = 8 * blocks + 2
        inner = tuple(range(width // 4 // SUB))
        received = received.reshape(count, tiles, sub, LANES).transpose(1, 0, 2, 3)
        received = received.reshape(tiles, len(inner), SUB, LANES).transpose(1, 0, 2, 3)
        received = received.reshape(len(inner), tiles * SUB, LANES)

    w_hi, w_lo = radix4_tables(width)
    res = resampler_tables()
    rows = ((frames + HALO) // 4 - 4 + SUB) // SUB * SUB
    made = pl.pallas_call(
        functools.partial(main_kernel, inner, frames),
        out_shape=jax.ShapeDtypeStruct((len(inner), rows_out, LANES), f32),
        in_specs=[vmem] * 6,
        out_specs=vmem,
        scratch_shapes=[
            pltpu.VMEM((4, frames + HALO, 2 * LANES), f32),
            pltpu.VMEM((8, frames + HALO + 16, LANES), f32),
            pltpu.VMEM((32, rows + SUB, LANES), f32),
            pltpu.VMEM((4, 10 * rows, LANES), bf16),
            pltpu.VMEM((4, 10 * rows, LANES), bf16),
            pltpu.VMEM((40, rows, LANES), f32),
            pltpu.VMEM((8, outs, LANES), f32),
            pltpu.VMEM((4, outs + 3 * (outs % LANES), 2 * LANES), bf16),
            pltpu.VMEM((4, outs, 2 * LANES), bf16),
        ],
        compiler_params=pltpu.CompilerParams(vmem_limit_bytes=24 << 20),
    )(received, w_hi, w_lo, res, synth_taps, analysis_taps)

    if tiled:
        back = exchange(made)
        out = pl.pallas_call(
            functools.partial(final_kernel, order),
            out_shape=jax.ShapeDtypeStruct((sub, 4, 2 * count * outs // LANES, LANES), f32),
            in_specs=[vmem],
            out_specs=hbm,
            scratch_shapes=[
                pltpu.VMEM((4, sub, 2 * count * outs // LANES, LANES), f32),
                pltpu.SemaphoreType.DMA((4,)),
            ],
            compiler_params=small,
        )(back)
        out = out.reshape(channels, count * outs // LANES, 2, LANES).transpose(0, 2, 1, 3)
        return out.reshape(channels, 2, count * outs)
    tiles = rows_out // SUB
    made = made.reshape(len(inner), tiles, SUB, LANES).transpose(1, 0, 2, 3)
    made = made.reshape(tiles, count, sub, LANES).transpose(1, 0, 2, 3)
    back = exchange(made[np.array(order)])
    back = back[np.argsort(np.array(order))]
    full = outs // LANES
    head = back[:, : 8 * full].reshape(count, full, 4, 2, sub, LANES).transpose(4, 2, 3, 0, 1, 5)
    head = head.reshape(channels, 2, count, full * LANES)
    rest = back[:, 8 * full :].reshape(count, 4, sub, 2, outs - full * LANES).transpose(2, 1, 3, 0, 4)
    rest = rest.reshape(channels, 2, count, -1)
    return jnp.concatenate([head, rest], axis=3).reshape(channels, 2, count * outs)


def solution(mesh):
    in_specs = (P("tm", "station", None), P(), P())
    out_specs = P("tm", "station", None)
    order = list(range(mesh.shape["tm"]))
    if len(order) == len(ORDER):
        order = ORDER
    return jax.shard_map(
        functools.partial(shards, order),
        mesh=mesh,
        in_specs=in_specs,
        out_specs=out_specs,
        check_vma=False,
    )
```

```python
import functools
import math

import jax
import jax.numpy as jnp
import numpy as np
from jax import lax
from jax.experimental import pallas as pl
from jax.experimental.pallas import tpu as pltpu
from jax.sharding import PartitionSpec as P

RT = 32
PHASES = 64
UP, DOWN = 5, 4
LANES = 128
SUB = 8
ORDERS = [
    [9, 3, 7, 13, 12, 8, 0, 4, 1, 15, 6, 14, 10, 2, 5, 11],
    [9, 10, 3, 13, 5, 12, 11, 0, 4, 1, 15, 6, 14, 7, 2, 8],
]
HALO = 32


def split(value):
    high = value.astype(jnp.bfloat16)
    low = (value - high.astype(jnp.float32)).astype(jnp.bfloat16)
    return high, low


def np_split(value):
    value = value.astype(np.float32)
    high = value.astype(jnp.bfloat16)
    low = (value - high.astype(np.float32)).astype(jnp.bfloat16)
    return high, low


def radix4_tables(width):
    quarter = width // 4
    k = np.arange(quarter)[:, None]
    m = np.arange(quarter)[None, :]
    blocks = []
    for r in range(4):
        angle = ((4 * k + r) * m % width) * (2.0 * math.pi / width)
        cosine = np.cos(angle) / math.sqrt(width)
        sine = np.sin(angle) / math.sqrt(width)
        blocks.append(np.block([[cosine, sine], [-sine, cosine]]))
    return np_split(np.stack(blocks))


def resampler_tables():
    parts = []
    for j in range(UP):
        sample = np.arange(LANES)[None, :] + LANES * j
        start = 128 * (min(j, 3) - 1)
        column = np.arange(2 * LANES)[:, None] + start
        lag = DOWN * sample // UP - column
        phase = PHASES * (DOWN * sample % UP) // UP
        offset = lag + phase / PHASES - (RT // 2 - 1)
        window = 0.5 + 0.5 * np.cos(math.pi * offset / (RT / 2.0))
        coeff = 0.9 * np.sinc(0.9 * offset) * window
        parts.append(np_split(np.where((lag >= 0) & (lag < RT), coeff, 0.0)))
    out = [np.concatenate([high, low], axis=1) for high, low in parts[:3]]
    out.append(np.concatenate([parts[3][0], parts[4][0]], axis=1))
    out.append(np.concatenate([parts[3][1], parts[4][1]], axis=1))
    return np.stack(out)


def lane_iota():
    return lax.broadcasted_iota(jnp.int32, (SUB, LANES), 1)


def prep_kernel(order, blocks, x_ref, o_ref, buf_ref, sems):
    sub, _, length, _ = x_ref.shape
    lane = lane_iota()
    copies = [
        pltpu.make_async_copy(x_ref.at[:, r], buf_ref.at[r], sems.at[r]) for r in range(4)
    ]
    for copy in copies:
        copy.start()
    for r in range(4):
        copies[r].wait()
        flat_ref = buf_ref.at[r].reshape(sub * length, LANES)
        for place, dev in enumerate(order):
            for lb in range(blocks):
                for part in range(2):
                    t = (r * blocks + lb) * 2 + part
                    row = 2 * (blocks * dev + lb) + part
                    o_ref[place, t * SUB : (t + 1) * SUB, :] = flat_ref[
                        pl.ds(row, SUB, stride=length), :
                    ]
    for place, dev in enumerate(order):
        for part in range(2):
            total = jnp.zeros((SUB, LANES), jnp.float32)
            if dev > 0:
                last = order.index(dev - 1)
                for r in range(4):
                    t = (r * blocks + blocks - 1) * 2 + part
                    value = o_ref[last, t * SUB : (t + 1) * SUB, :]
                    if r < 3:
                        value = pltpu.roll(value, HALO * (r + 1), 1)
                    total = jnp.where(lane // HALO == r, value, total)
            t = 8 * blocks + part
            o_ref[place, t * SUB : (t + 1) * SUB, :] = total


def main_kernel(
    inputs, order, frames, x_ref, w_hi, w_lo, res_ref, st_ref, at_ref, o_ref,
    a_ref, v_ref, y_ref, yh_ref, yl_ref, z_ref, u_ref, bh_ref, bl_ref,
):
    blocks = frames // LANES
    count = len(inputs)
    place_of = {dev: place for place, dev in enumerate(inputs)}
    f32 = jnp.float32

    def dot(a, b):
        return lax.dot_general(a, b, (((1,), (0,)), ((), ())), preferred_element_type=f32)

    def dot_t(a, b):
        return lax.dot_general(a, b, (((1,), (1,)), ((), ())), preferred_element_type=f32)

    def tile(t):
        return jnp.concatenate(
            [x_ref[place_of[s], t * SUB : (t + 1) * SUB, :] for s in range(count)], axis=0
        )

    halo = [tile(8 * blocks + part).T for part in range(2)]
    for r in range(4):
        rows = [jnp.concatenate([h[r * HALO : (r + 1) * HALO] for h in halo], axis=1)]
        for lb in range(blocks):
            rows.append(
                jnp.concatenate([tile((r * blocks + lb) * 2 + part).T for part in range(2)], axis=1)
            )
        high, low = split(jnp.concatenate(rows, axis=0))
        a_ref[r] = dot(high, w_hi[r]) + dot(low, w_hi[r]) + dot(high, w_lo[r])

    total = frames + HALO

    @pl.loop(0, total // 16, unroll=3)
    def _(i):
        row = pl.ds(pl.multiple_of(i * 16, 16), 16)
        re = [a_ref[r, row, :LANES] for r in range(4)]
        im = [a_ref[r, row, LANES:] for r in range(4)]
        sr, dr = re[0] + re[2], re[0] - re[2]
        si, di = im[0] + im[2], im[0] - im[2]
        tr, er = re[1] + re[3], re[1] - re[3]
        ti, ei = im[1] + im[3], im[1] - im[3]
        v_ref[0, row, :] = sr + tr
        v_ref[4, row, :] = si + ti
        v_ref[1, row, :] = dr - ei
        v_ref[5, row, :] = di + er
        v_ref[2, row, :] = sr - tr
        v_ref[6, row, :] = si - ti
        v_ref[3, row, :] = dr + ei
        v_ref[7, row, :] = di - er

    for k in range(8):
        v_ref[k, total : total + 16, :] = jnp.zeros((16, LANES), f32)
        y_ref[k * 2, 0:SUB, :] = jnp.zeros((SUB, LANES), f32)
        y_ref[k * 2 + 1, 0:SUB, :] = jnp.zeros((SUB, LANES), f32)
        y_ref[16 + k * 2, 0:SUB, :] = jnp.zeros((SUB, LANES), f32)
        y_ref[16 + k * 2 + 1, 0:SUB, :] = jnp.zeros((SUB, LANES), f32)

    taps_len = st_ref.shape[0]
    groups = (total // 4 - 4 + SUB) // SUB
    for q in range(4):

        def step(t, q=q):
            base = t * 32 + 16
            accs = {}
            vals = {}

            def load(part, j):
                vals[part, j] = v_ref[part * 4 + q, pl.ds(base + j, SUB, stride=4), :]

            for part in range(2):
                for j in range(1, 4):
                    load(part, j)
            for p in range(taps_len):
                tap = jnp.broadcast_to(
                    st_ref[p : p + 1, q * LANES : (q + 1) * LANES], (SUB, LANES)
                )
                for part in range(2):
                    load(part, -p)
                    for b in range(4):
                        term = tap * vals[part, b - p]
                        accs[part, b] = term if p == 0 else accs[part, b] + term
            for part in range(2):
                for b in range(4):
                    row = pl.ds(t * SUB + SUB, SUB) if isinstance(t, int) else pl.ds(pl.multiple_of(t * SUB, SUB) + SUB, SUB)
                    y_ref[part * 16 + b * 4 + q, row, :] = accs[part, b]

        if q == 3:
            for t in range(groups):
                step(t)
        else:
            pl.loop(0, groups, unroll=3)(step)


    rows = groups * SUB
    both = 2 * rows
    for b in range(4):
        for q in range(4):
            value = jnp.concatenate(
                [y_ref[part * 16 + b * 4 + q, SUB : SUB + rows, :] for part in range(2)], axis=0
            )
            high, low = split(value)
            first = b * both + (both if q == 3 else 0)
            yh_ref[q, first : first + both, :] = high
            yl_ref[q, first : first + both, :] = low
    value = jnp.concatenate(
        [y_ref[part * 16 + 15, SUB - 1 : SUB - 1 + rows, :] for part in range(2)], axis=0
    )
    high, low = split(value)
    yh_ref[3, 0:both, :] = high
    yl_ref[3, 0:both, :] = low

    def store_z(j, value):
        for b in range(4):
            g, q = (5 * b + j) // 4, (5 * b + j) % 4
            for part in range(2):
                first = b * both + part * rows
                z_ref[part * 20 + g * 4 + q] = value[first : first + rows]

    def pair(ref, left, right):
        first = both if left == 2 else 0
        a = ref[3, 0 : 4 * both] if left < 0 else ref[left, 0 : 4 * both]
        return jnp.concatenate([a, ref[right, first if right == 3 else 0 : (first if right == 3 else 0) + 4 * both]], axis=1)

    for j in range(3):
        high = pair(yh_ref, j - 1, j)
        low = pair(yl_ref, j - 1, j)
        wide = dot(high, res_ref[j])
        store_z(j, wide[:, :LANES] + wide[:, LANES:] + dot(low, res_ref[j, :, :LANES]))
    high = pair(yh_ref, 2, 3)
    low = pair(yl_ref, 2, 3)
    wide = dot(high, res_ref[3]) + dot(high, res_ref[4]) + dot(low, res_ref[3])
    store_z(3, wide[:, :LANES])
    store_z(4, wide[:, LANES:])

    outs = frames * UP // DOWN
    taps_len = at_ref.shape[0]
    groups2 = frames // 4 // SUB
    for q in range(4):

        def step(t, q=q):
            accs = {}
            vals = {}

            def load(part, j):
                shift = j // UP
                slot = part * 20 + (j - UP * shift) * 4 + q
                vals[part, j] = z_ref[slot, pl.ds(t * SUB + 4 + shift, SUB), :]

            for part in range(2):
                for j in range(1, UP):
                    load(part, j)
            for p in range(taps_len):
                tap = jnp.broadcast_to(
                    at_ref[p : p + 1, q * LANES : (q + 1) * LANES], (SUB, LANES)
                )
                for part in range(2):
                    load(part, -p)
                    for g in range(UP):
                        term = tap * vals[part, g - p]
                        accs[part, g] = term if p == 0 else accs[part, g] + term
            for part in range(2):
                for g in range(UP):
                    row = pl.ds(t * SUB * UP + g, SUB, stride=UP)
                    u_ref[part * 4 + q, row, :] = accs[part, g]

        if q == 0:
            for t in range(groups2):
                step(t)
        else:
            pl.loop(0, groups2, unroll=2)(step)


    @pl.loop(0, outs // 16, unroll=4)
    def _(i):
        row = pl.ds(pl.multiple_of(i * 16, 16), 16)
        re = [u_ref[q, row, :] for q in range(4)]
        im = [u_ref[4 + q, row, :] for q in range(4)]
        sr, dr = re[0] + re[2], re[0] - re[2]
        si, di = im[0] + im[2], im[0] - im[2]
        tr, er = re[1] + re[3], re[1] - re[3]
        ti, ei = im[1] + im[3], im[1] - im[3]
        spectra = [
            (sr + tr, si + ti), (dr + ei, di - er), (sr - tr, si - ti), (dr - ei, di + er)
        ]
        for r in range(4):
            for part in range(2):
                high, low = split(spectra[r][part])
                cols = slice(part * LANES, (part + 1) * LANES)
                bh_ref[r, row, cols] = high
                bl_ref[r, row, cols] = low

    lane = lax.broadcasted_iota(jnp.int32, (LANES, LANES), 1)
    full = outs // LANES
    rest = outs - full * LANES
    for r in range(4):
        for place in range(2):
            first = full * LANES + place * rest
            last = slice(full * LANES, full * LANES + rest)
            if place == 1:
                bh_ref[r, first : first + rest] = bh_ref[r, last]
            bh_ref[r, first + LANES : first + LANES + rest] = bl_ref[r, last]
        main = slice(0, full * LANES)
        high, low = bh_ref[r, main], bl_ref[r, main]
        out = dot_t(w_hi[r], high) + dot_t(w_hi[r], low) + dot_t(w_lo[r], high)
        tail = dot_t(w_hi[r], bh_ref[r, full * LANES :])
        tail = tail[:, :LANES] + tail[:, LANES:]
        tail = tail + dot_t(w_lo[r], bh_ref[r, full * LANES : (full + 1) * LANES])
        for part in range(2):
            for k in range(full):
                t = k * SUB + r * 2 + part
                value = out[part * LANES : (part + 1) * LANES, k * LANES : (k + 1) * LANES]
                for place, dev in enumerate(order):
                    o_ref[place, t * SUB : (t + 1) * SUB, :] = value[dev * SUB : (dev + 1) * SUB]
        value = jnp.where(lane < rest, tail[:LANES], tail[LANES:])
        t = full * SUB + r
        for place, dev in enumerate(order):
            o_ref[place, t * SUB : (t + 1) * SUB, :] = value[dev * SUB : (dev + 1) * SUB]


def final_kernel(order, x_ref, o_ref, buf_ref, sems):
    _, _, length, _ = o_ref.shape
    lane = lane_iota()
    half = LANES // 2
    place_of = {dev: place for place, dev in enumerate(order)}
    copies = []

    def tile(dev, t):
        return x_ref[place_of[dev], t * SUB : (t + 1) * SUB, :]

    for r in range(4):
        flat_ref = buf_ref.at[r].reshape(SUB * length, LANES)
        for dev in range(0, len(order), 2):
            for part in range(2):
                t = r * 2 + part
                ends = [tile(dev, 16 + r), tile(dev + 1, 16 + r)]
                ends[1 - part] = pltpu.roll(ends[1 - part], half, 1)
                r0 = pltpu.roll(tile(dev + 1, t), half, 1)
                r1 = pltpu.roll(tile(dev + 1, 8 + t), half, 1)
                values = [
                    tile(dev, t),
                    tile(dev, 8 + t),
                    jnp.where(lane < half, ends[0], r0),
                    jnp.where(lane < half, r0, r1),
                    jnp.where(lane < half, r1, ends[1]),
                ]
                for k, value in enumerate(values):
                    first = (5 * (dev // 2) + k) * 2 + part
                    flat_ref[pl.ds(first, SUB, stride=length), :] = value
        copies.append(pltpu.make_async_copy(buf_ref.at[r], o_ref.at[:, r], sems.at[r]))
        copies[-1].start()
    for copy in copies:
        copy.wait()


def shards(order_in, order_out, spectra, synth_taps, analysis_taps):
    count = lax.axis_size("tm")
    channels, parts, length = spectra.shape
    width = channels * count
    frames = length // count
    outs = frames * UP // DOWN
    blocks = frames // LANES
    tiled = channels == 4 * SUB
    vmem = pl.BlockSpec(memory_space=pltpu.VMEM)
    hbm = pl.BlockSpec(memory_space=pltpu.HBM)
    f32, bf16 = jnp.float32, jnp.bfloat16
    rows_in = 8 * blocks * SUB + 2 * SUB
    rows_out = (outs * 64) // LANES
    sub = channels // 4
    small = pltpu.CompilerParams(vmem_limit_bytes=8 << 20)

    def exchange(value, order):
        return lax.all_to_all(
            value, "tm", split_axis=0, concat_axis=0, tiled=True, axis_index_groups=[list(order)]
        )

    if tiled:
        flat = spectra.reshape(channels, 2, length // LANES, LANES).transpose(0, 2, 1, 3)
        flat = flat.reshape(sub, 4, -1, LANES)
        flat = pltpu.with_memory_space_constraint(flat, pltpu.HBM)
        sent = pl.pallas_call(
            functools.partial(prep_kernel, order_in, blocks),
            out_shape=jax.ShapeDtypeStruct((count, rows_in, LANES), f32),
            in_specs=[hbm],
            out_specs=vmem,
            scratch_shapes=[
                pltpu.VMEM((4, sub) + flat.shape[2:], f32),
                pltpu.SemaphoreType.DMA((4,)),
            ],
            compiler_params=small,
        )(flat)
        received = exchange(sent, order_in)
        inner = (order_in, order_out)
    else:
        cut = spectra.reshape(sub, 4, 2, count, blocks, LANES).transpose(3, 1, 4, 2, 0, 5)
        tail = spectra.reshape(sub, 4, 2, count, frames)[..., frames - HALO :]
        tail = jnp.concatenate([jnp.zeros_like(tail[..., :1, :]), tail[..., :-1, :]], axis=3)
        tail = tail.transpose(3, 2, 0, 1, 4).reshape(count, 2 * sub, LANES)
        sent = jnp.concatenate([cut.reshape(count, 8 * blocks * sub, LANES), tail], axis=1)
        received = exchange(sent, range(count))
        tiles = 8 * blocks + 2
        inner = (range(width // 4 // SUB),) * 2
        received = received.reshape(count, tiles, sub, LANES).transpose(1, 0, 2, 3)
        received = received.reshape(tiles, len(inner[0]), SUB, LANES).transpose(1, 0, 2, 3)
        received = received.reshape(len(inner[0]), tiles * SUB, LANES)

    w_hi, w_lo = radix4_tables(width)
    res = resampler_tables()
    rows = ((frames + HALO) // 4 - 4 + SUB) // SUB * SUB
    made = pl.pallas_call(
        functools.partial(main_kernel, *inner, frames),
        out_shape=jax.ShapeDtypeStruct((len(inner[0]), rows_out, LANES), f32),
        in_specs=[vmem] * 6,
        out_specs=vmem,
        scratch_shapes=[
            pltpu.VMEM((4, frames + HALO, 2 * LANES), f32),
            pltpu.VMEM((8, frames + HALO + 16, LANES), f32),
            pltpu.VMEM((32, rows + SUB, LANES), f32),
            pltpu.VMEM((4, 10 * rows, LANES), bf16),
            pltpu.VMEM((4, 10 * rows, LANES), bf16),
            pltpu.VMEM((40, rows, LANES), f32),
            pltpu.VMEM((8, outs, LANES), f32),
            pltpu.VMEM((4, outs + 3 * (outs % LANES), 2 * LANES), bf16),
            pltpu.VMEM((4, outs, 2 * LANES), bf16),
        ],
        compiler_params=pltpu.CompilerParams(vmem_limit_bytes=24 << 20),
    )(received, w_hi, w_lo, res, synth_taps, analysis_taps)

    if tiled:
        back = exchange(made, order_out)
        out = pl.pallas_call(
            functools.partial(final_kernel, order_out),
            out_shape=jax.ShapeDtypeStruct((sub, 4, 2 * count * outs // LANES, LANES), f32),
            in_specs=[vmem],
            out_specs=hbm,
            scratch_shapes=[
                pltpu.VMEM((4, sub, 2 * count * outs // LANES, LANES), f32),
                pltpu.SemaphoreType.DMA((4,)),
            ],
            compiler_params=small,
        )(back)
        out = out.reshape(channels, count * outs // LANES, 2, LANES).transpose(0, 2, 1, 3)
        return out.reshape(channels, 2, count * outs)
    tiles = rows_out // SUB
    made = made.reshape(len(inner[0]), tiles, SUB, LANES).transpose(1, 0, 2, 3)
    made = made.reshape(tiles, count, sub, LANES).transpose(1, 0, 2, 3)
    back = exchange(made, range(count))
    full = outs // LANES
    head = back[:, : 8 * full].reshape(count, full, 4, 2, sub, LANES).transpose(4, 2, 3, 0, 1, 5)
    head = head.reshape(channels, 2, count, full * LANES)
    rest = back[:, 8 * full :].reshape(count, 4, sub, 2, outs - full * LANES).transpose(2, 1, 3, 0, 4)
    rest = rest.reshape(channels, 2, count, -1)
    return jnp.concatenate([head, rest], axis=3).reshape(channels, 2, count * outs)


def solution(mesh):
    in_specs = (P("tm", "station", None), P(), P())
    out_specs = P("tm", "station", None)
    orders = [list(range(mesh.shape["tm"]))] * 2
    if len(orders[0]) == len(ORDERS[0]):
        orders = ORDERS
    return jax.shard_map(
        functools.partial(shards, *orders),
        mesh=mesh,
        in_specs=in_specs,
        out_specs=out_specs,
        check_vma=False,
    )
```

```python
import functools
import math

import jax
import jax.numpy as jnp
import numpy as np
from jax import lax
from jax.experimental import pallas as pl
from jax.experimental.pallas import tpu as pltpu
from jax.sharding import PartitionSpec as P

RT = 32
PHASES = 64
UP, DOWN = 5, 4
LANES = 128
SUB = 8
ORDERS = [
    [9, 3, 7, 13, 12, 8, 11, 0, 4, 1, 15, 6, 14, 10, 2, 5],
    [9, 10, 6, 5, 13, 12, 11, 0, 4, 1, 15, 3, 14, 7, 2, 8],
]
HALO = 32


def split(value):
    high = value.astype(jnp.bfloat16)
    low = (value - high.astype(jnp.float32)).astype(jnp.bfloat16)
    return high, low


def np_split(value):
    value = value.astype(np.float32)
    high = value.astype(jnp.bfloat16)
    low = (value - high.astype(np.float32)).astype(jnp.bfloat16)
    return high, low


def radix4_tables(width):
    quarter = width // 4
    k = np.arange(quarter)[:, None]
    m = np.arange(quarter)[None, :]
    blocks = []
    for r in range(4):
        angle = ((4 * k + r) * m % width) * (2.0 * math.pi / width)
        cosine = np.cos(angle) / math.sqrt(width)
        sine = np.sin(angle) / math.sqrt(width)
        blocks.append(np.block([[cosine, sine], [-sine, cosine]]))
    return np_split(np.stack(blocks))


def resampler_tables():
    parts = []
    for j in range(UP):
        sample = np.arange(LANES)[None, :] + LANES * j
        start = 128 * (min(j, 3) - 1)
        column = np.arange(2 * LANES)[:, None] + start
        lag = DOWN * sample // UP - column
        phase = PHASES * (DOWN * sample % UP) // UP
        offset = lag + phase / PHASES - (RT // 2 - 1)
        window = 0.5 + 0.5 * np.cos(math.pi * offset / (RT / 2.0))
        coeff = 0.9 * np.sinc(0.9 * offset) * window
        parts.append(np_split(np.where((lag >= 0) & (lag < RT), coeff, 0.0)))
    out = [np.concatenate([high, low], axis=1) for high, low in parts[:3]]
    out.append(np.concatenate([parts[3][0], parts[4][0]], axis=1))
    out.append(np.concatenate([parts[3][1], parts[4][1]], axis=1))
    return np.stack(out)


def pitched(rows):
    return (rows // SUB // 2 * 2 + 1) * SUB if rows // SUB % 2 == 0 else rows


def lane_iota():
    return lax.broadcasted_iota(jnp.int32, (SUB, LANES), 1)


def prep_kernel(order, blocks, x_ref, o_ref, buf_ref, sems):
    sub, _, length, _ = x_ref.shape
    lane = lane_iota()
    copies = [
        pltpu.make_async_copy(x_ref.at[:, r], buf_ref.at[r, :, 0:length], sems.at[r]) for r in range(4)
    ]
    for copy in copies:
        copy.start()
    for r in range(4):
        copies[r].wait()
        pitch = buf_ref.shape[2]
        flat_ref = buf_ref.at[r].reshape(sub * pitch, LANES)
        for place, dev in enumerate(order):
            for lb in range(blocks):
                for part in range(2):
                    t = (r * blocks + lb) * 2 + part
                    row = 2 * (blocks * dev + lb) + part
                    o_ref[place, t * SUB : (t + 1) * SUB, :] = flat_ref[
                        pl.ds(row, SUB, stride=pitch), :
                    ]
    for place, dev in enumerate(order):
        for part in range(2):
            total = jnp.zeros((SUB, LANES), jnp.float32)
            if dev > 0:
                last = order.index(dev - 1)
                for r in range(4):
                    t = (r * blocks + blocks - 1) * 2 + part
                    value = o_ref[last, t * SUB : (t + 1) * SUB, :]
                    if r < 3:
                        value = pltpu.roll(value, HALO * (r + 1), 1)
                    total = jnp.where(lane // HALO == r, value, total)
            t = 8 * blocks + part
            o_ref[place, t * SUB : (t + 1) * SUB, :] = total


def main_kernel(
    inputs, order, frames, x_ref, w_hi, w_lo, res_ref, st_ref, at_ref, o_ref,
    a_ref, v_ref, y_ref, yh_ref, yl_ref, z_ref, u_ref, bh_ref, bl_ref,
):
    blocks = frames // LANES
    count = len(inputs)
    place_of = {dev: place for place, dev in enumerate(inputs)}
    f32 = jnp.float32

    def dot(a, b):
        return lax.dot_general(a, b, (((1,), (0,)), ((), ())), preferred_element_type=f32)

    def dot_t(a, b):
        return lax.dot_general(a, b, (((1,), (1,)), ((), ())), preferred_element_type=f32)

    def tile(t):
        return jnp.concatenate(
            [x_ref[place_of[s], t * SUB : (t + 1) * SUB, :] for s in range(count)], axis=0
        )

    halo = [tile(8 * blocks + part).T for part in range(2)]
    for r in range(4):
        rows = [jnp.concatenate([h[r * HALO : (r + 1) * HALO] for h in halo], axis=1)]
        for lb in range(blocks):
            rows.append(
                jnp.concatenate([tile((r * blocks + lb) * 2 + part).T for part in range(2)], axis=1)
            )
        high, low = split(jnp.concatenate(rows, axis=0))
        a_ref[r] = dot(high, w_hi[r]) + dot(low, w_hi[r]) + dot(high, w_lo[r])

    total = frames + HALO

    @pl.loop(0, total // 16, unroll=3)
    def _(i):
        row = pl.ds(pl.multiple_of(i * 16, 16), 16)
        re = [a_ref[r, row, :LANES] for r in range(4)]
        im = [a_ref[r, row, LANES:] for r in range(4)]
        sr, dr = re[0] + re[2], re[0] - re[2]
        si, di = im[0] + im[2], im[0] - im[2]
        tr, er = re[1] + re[3], re[1] - re[3]
        ti, ei = im[1] + im[3], im[1] - im[3]
        v_ref[0, row, :] = sr + tr
        v_ref[4, row, :] = si + ti
        v_ref[1, row, :] = dr - ei
        v_ref[5, row, :] = di + er
        v_ref[2, row, :] = sr - tr
        v_ref[6, row, :] = si - ti
        v_ref[3, row, :] = dr + ei
        v_ref[7, row, :] = di - er

    for k in range(8):
        v_ref[k, total : total + 16, :] = jnp.zeros((16, LANES), f32)
        y_ref[k * 2, 0:SUB, :] = jnp.zeros((SUB, LANES), f32)
        y_ref[k * 2 + 1, 0:SUB, :] = jnp.zeros((SUB, LANES), f32)
        y_ref[16 + k * 2, 0:SUB, :] = jnp.zeros((SUB, LANES), f32)
        y_ref[16 + k * 2 + 1, 0:SUB, :] = jnp.zeros((SUB, LANES), f32)

    taps_len = st_ref.shape[0]
    groups = (total // 4 - 4 + SUB) // SUB
    for q in range(4):

        def step(t, q=q):
            base = t * 32 + 16
            accs = {}
            vals = {}

            def load(part, j):
                vals[part, j] = v_ref[part * 4 + q, pl.ds(base + j, SUB, stride=4), :]

            for part in range(2):
                for j in range(1, 4):
                    load(part, j)
            for p in range(taps_len):
                tap = jnp.broadcast_to(
                    st_ref[p : p + 1, q * LANES : (q + 1) * LANES], (SUB, LANES)
                )
                for part in range(2):
                    load(part, -p)
                    for b in range(4):
                        term = tap * vals[part, b - p]
                        accs[part, b] = term if p == 0 else accs[part, b] + term
            for part in range(2):
                for b in range(4):
                    row = pl.ds(t * SUB + SUB, SUB) if isinstance(t, int) else pl.ds(pl.multiple_of(t * SUB, SUB) + SUB, SUB)
                    y_ref[part * 16 + b * 4 + q, row, :] = accs[part, b]

        if q == 3:
            for t in range(groups):
                step(t)
        else:
            pl.loop(0, groups, unroll=3)(step)


    rows = groups * SUB
    both = 2 * rows
    for b in range(4):
        for q in range(4):
            value = jnp.concatenate(
                [y_ref[part * 16 + b * 4 + q, SUB : SUB + rows, :] for part in range(2)], axis=0
            )
            high, low = split(value)
            first = b * both + (both if q == 3 else 0)
            yh_ref[q, first : first + both, :] = high
            yl_ref[q, first : first + both, :] = low
    value = jnp.concatenate(
        [y_ref[part * 16 + 15, SUB - 1 : SUB - 1 + rows, :] for part in range(2)], axis=0
    )
    high, low = split(value)
    yh_ref[3, 0:both, :] = high
    yl_ref[3, 0:both, :] = low

    def store_z(j, value):
        for b in range(4):
            g, q = (5 * b + j) // 4, (5 * b + j) % 4
            for part in range(2):
                first = b * both + part * rows
                z_ref[part * 20 + g * 4 + q] = value[first : first + rows]

    def pair(ref, left, right):
        first = both if left == 2 else 0
        a = ref[3, 0 : 4 * both] if left < 0 else ref[left, 0 : 4 * both]
        return jnp.concatenate([a, ref[right, first if right == 3 else 0 : (first if right == 3 else 0) + 4 * both]], axis=1)

    for j in range(3):
        high = pair(yh_ref, j - 1, j)
        low = pair(yl_ref, j - 1, j)
        wide = dot(high, res_ref[j])
        store_z(j, wide[:, :LANES] + wide[:, LANES:] + dot(low, res_ref[j, :, :LANES]))
    high = pair(yh_ref, 2, 3)
    low = pair(yl_ref, 2, 3)
    wide = dot(high, res_ref[3]) + dot(high, res_ref[4]) + dot(low, res_ref[3])
    store_z(3, wide[:, :LANES])
    store_z(4, wide[:, LANES:])

    outs = frames * UP // DOWN
    taps_len = at_ref.shape[0]
    groups2 = frames // 4 // SUB
    for q in range(4):

        def step(t, q=q):
            accs = {}
            vals = {}

            def load(part, j):
                shift = j // UP
                slot = part * 20 + (j - UP * shift) * 4 + q
                vals[part, j] = z_ref[slot, pl.ds(t * SUB + 4 + shift, SUB), :]

            for part in range(2):
                for j in range(1, UP):
                    load(part, j)
            for p in range(taps_len):
                tap = jnp.broadcast_to(
                    at_ref[p : p + 1, q * LANES : (q + 1) * LANES], (SUB, LANES)
                )
                for part in range(2):
                    load(part, -p)
                    for g in range(UP):
                        term = tap * vals[part, g - p]
                        accs[part, g] = term if p == 0 else accs[part, g] + term
            for part in range(2):
                for g in range(UP):
                    row = pl.ds(t * SUB * UP + g, SUB, stride=UP)
                    u_ref[part * 4 + q, row, :] = accs[part, g]

        if q == 0:
            for t in range(groups2):
                step(t)
        else:
            pl.loop(0, groups2, unroll=2)(step)


    @pl.loop(0, outs // 16, unroll=4)
    def _(i):
        row = pl.ds(pl.multiple_of(i * 16, 16), 16)
        re = [u_ref[q, row, :] for q in range(4)]
        im = [u_ref[4 + q, row, :] for q in range(4)]
        sr, dr = re[0] + re[2], re[0] - re[2]
        si, di = im[0] + im[2], im[0] - im[2]
        tr, er = re[1] + re[3], re[1] - re[3]
        ti, ei = im[1] + im[3], im[1] - im[3]
        spectra = [
            (sr + tr, si + ti), (dr + ei, di - er), (sr - tr, si - ti), (dr - ei, di + er)
        ]
        for r in range(4):
            for part in range(2):
                high, low = split(spectra[r][part])
                cols = slice(part * LANES, (part + 1) * LANES)
                bh_ref[r, row, cols] = high
                bl_ref[r, row, cols] = low

    lane = lax.broadcasted_iota(jnp.int32, (LANES, LANES), 1)
    full = outs // LANES
    rest = outs - full * LANES
    for r in range(4):
        for place in range(2):
            first = full * LANES + place * rest
            last = slice(full * LANES, full * LANES + rest)
            if place == 1:
                bh_ref[r, first : first + rest] = bh_ref[r, last]
            bh_ref[r, first + LANES : first + LANES + rest] = bl_ref[r, last]
        main = slice(0, full * LANES)
        high, low = bh_ref[r, main], bl_ref[r, main]
        out = dot_t(w_hi[r], high) + dot_t(w_hi[r], low) + dot_t(w_lo[r], high)
        tail = dot_t(w_hi[r], bh_ref[r, full * LANES :])
        tail = tail[:, :LANES] + tail[:, LANES:]
        tail = tail + dot_t(w_lo[r], bh_ref[r, full * LANES : (full + 1) * LANES])
        for part in range(2):
            for k in range(full):
                t = k * SUB + r * 2 + part
                value = out[part * LANES : (part + 1) * LANES, k * LANES : (k + 1) * LANES]
                for place, dev in enumerate(order):
                    o_ref[place, t * SUB : (t + 1) * SUB, :] = value[dev * SUB : (dev + 1) * SUB]
        value = jnp.where(lane < rest, tail[:LANES], tail[LANES:])
        t = full * SUB + r
        for place, dev in enumerate(order):
            o_ref[place, t * SUB : (t + 1) * SUB, :] = value[dev * SUB : (dev + 1) * SUB]


def final_kernel(order, x_ref, o_ref, buf_ref, sems):
    _, _, length, _ = o_ref.shape
    lane = lane_iota()
    half = LANES // 2
    place_of = {dev: place for place, dev in enumerate(order)}
    copies = []

    def tile(dev, t):
        return x_ref[place_of[dev], t * SUB : (t + 1) * SUB, :]

    for r in range(4):
        pitch = buf_ref.shape[2]
        flat_ref = buf_ref.at[r].reshape(SUB * pitch, LANES)
        for dev in range(0, len(order), 2):
            for part in range(2):
                t = r * 2 + part
                ends = [tile(dev, 16 + r), tile(dev + 1, 16 + r)]
                ends[1 - part] = pltpu.roll(ends[1 - part], half, 1)
                r0 = pltpu.roll(tile(dev + 1, t), half, 1)
                r1 = pltpu.roll(tile(dev + 1, 8 + t), half, 1)
                values = [
                    tile(dev, t),
                    tile(dev, 8 + t),
                    jnp.where(lane < half, ends[0], r0),
                    jnp.where(lane < half, r0, r1),
                    jnp.where(lane < half, r1, ends[1]),
                ]
                for k, value in enumerate(values):
                    first = (5 * (dev // 2) + k) * 2 + part
                    flat_ref[pl.ds(first, SUB, stride=pitch), :] = value
        copies.append(pltpu.make_async_copy(buf_ref.at[r, :, 0:length], o_ref.at[:, r], sems.at[r]))
        copies[-1].start()
    for copy in copies:
        copy.wait()


def shards(order_in, order_out, spectra, synth_taps, analysis_taps):
    count = lax.axis_size("tm")
    channels, parts, length = spectra.shape
    width = channels * count
    frames = length // count
    outs = frames * UP // DOWN
    blocks = frames // LANES
    tiled = channels == 4 * SUB
    vmem = pl.BlockSpec(memory_space=pltpu.VMEM)
    hbm = pl.BlockSpec(memory_space=pltpu.HBM)
    f32, bf16 = jnp.float32, jnp.bfloat16
    rows_in = 8 * blocks * SUB + 2 * SUB
    rows_out = (outs * 64) // LANES
    sub = channels // 4
    small = pltpu.CompilerParams(vmem_limit_bytes=8 << 20)

    def exchange(value, order):
        return lax.all_to_all(
            value, "tm", split_axis=0, concat_axis=0, tiled=True, axis_index_groups=[list(order)]
        )

    if tiled:
        flat = spectra.reshape(channels, 2, length // LANES, LANES).transpose(0, 2, 1, 3)
        flat = flat.reshape(sub, 4, -1, LANES)
        flat = pltpu.with_memory_space_constraint(flat, pltpu.HBM)
        sent = pl.pallas_call(
            functools.partial(prep_kernel, order_in, blocks),
            out_shape=jax.ShapeDtypeStruct((count, rows_in, LANES), f32),
            in_specs=[hbm],
            out_specs=vmem,
            scratch_shapes=[
                pltpu.VMEM((4, sub, pitched(flat.shape[2]), LANES), f32),
                pltpu.SemaphoreType.DMA((4,)),
            ],
            compiler_params=small,
        )(flat)
        received = exchange(sent, order_in)
        inner = (order_in, order_out)
    else:
        cut = spectra.reshape(sub, 4, 2, count, blocks, LANES).transpose(3, 1, 4, 2, 0, 5)
        tail = spectra.reshape(sub, 4, 2, count, frames)[..., frames - HALO :]
        tail = jnp.concatenate([jnp.zeros_like(tail[..., :1, :]), tail[..., :-1, :]], axis=3)
        tail = tail.transpose(3, 2, 0, 1, 4).reshape(count, 2 * sub, LANES)
        sent = jnp.concatenate([cut.reshape(count, 8 * blocks * sub, LANES), tail], axis=1)
        received = exchange(sent, range(count))
        tiles = 8 * blocks + 2
        inner = (range(width // 4 // SUB),) * 2
        received = received.reshape(count, tiles, sub, LANES).transpose(1, 0, 2, 3)
        received = received.reshape(tiles, len(inner[0]), SUB, LANES).transpose(1, 0, 2, 3)
        received = received.reshape(len(inner[0]), tiles * SUB, LANES)

    w_hi, w_lo = radix4_tables(width)
    res = resampler_tables()
    rows = ((frames + HALO) // 4 - 4 + SUB) // SUB * SUB
    made = pl.pallas_call(
        functools.partial(main_kernel, *inner, frames),
        out_shape=jax.ShapeDtypeStruct((len(inner[0]), rows_out, LANES), f32),
        in_specs=[vmem] * 6,
        out_specs=vmem,
        scratch_shapes=[
            pltpu.VMEM((4, frames + HALO, 2 * LANES), f32),
            pltpu.VMEM((8, frames + HALO + 16, LANES), f32),
            pltpu.VMEM((32, rows + SUB, LANES), f32),
            pltpu.VMEM((4, 10 * rows, LANES), bf16),
            pltpu.VMEM((4, 10 * rows, LANES), bf16),
            pltpu.VMEM((40, rows, LANES), f32),
            pltpu.VMEM((8, outs, LANES), f32),
            pltpu.VMEM((4, outs + 3 * (outs % LANES), 2 * LANES), bf16),
            pltpu.VMEM((4, outs, 2 * LANES), bf16),
        ],
        compiler_params=pltpu.CompilerParams(vmem_limit_bytes=24 << 20),
    )(received, w_hi, w_lo, res, synth_taps, analysis_taps)

    if tiled:
        back = exchange(made, order_out)
        out = pl.pallas_call(
            functools.partial(final_kernel, order_out),
            out_shape=jax.ShapeDtypeStruct((sub, 4, 2 * count * outs // LANES, LANES), f32),
            in_specs=[vmem],
            out_specs=hbm,
            scratch_shapes=[
                pltpu.VMEM((4, sub, pitched(2 * count * outs // LANES), LANES), f32),
                pltpu.SemaphoreType.DMA((4,)),
            ],
            compiler_params=small,
        )(back)
        out = out.reshape(channels, count * outs // LANES, 2, LANES).transpose(0, 2, 1, 3)
        return out.reshape(channels, 2, count * outs)
    tiles = rows_out // SUB
    made = made.reshape(len(inner[0]), tiles, SUB, LANES).transpose(1, 0, 2, 3)
    made = made.reshape(tiles, count, sub, LANES).transpose(1, 0, 2, 3)
    back = exchange(made, range(count))
    full = outs // LANES
    head = back[:, : 8 * full].reshape(count, full, 4, 2, sub, LANES).transpose(4, 2, 3, 0, 1, 5)
    head = head.reshape(channels, 2, count, full * LANES)
    rest = back[:, 8 * full :].reshape(count, 4, sub, 2, outs - full * LANES).transpose(2, 1, 3, 0, 4)
    rest = rest.reshape(channels, 2, count, -1)
    return jnp.concatenate([head, rest], axis=3).reshape(channels, 2, count * outs)


def solution(mesh):
    in_specs = (P("tm", "station", None), P(), P())
    out_specs = P("tm", "station", None)
    orders = [list(range(mesh.shape["tm"]))] * 2
    if len(orders[0]) == len(ORDERS[0]):
        orders = ORDERS
    return jax.shard_map(
        functools.partial(shards, *orders),
        mesh=mesh,
        in_specs=in_specs,
        out_specs=out_specs,
        check_vma=False,
    )
```

```python
import functools
import math

import jax
import jax.numpy as jnp
import numpy as np
from jax import lax
from jax.experimental import pallas as pl
from jax.experimental.pallas import tpu as pltpu
from jax.sharding import PartitionSpec as P

RT = 32
PHASES = 64
UP, DOWN = 5, 4
LANES = 128
SUB = 8
ORDERS = [
    [9, 3, 7, 13, 12, 8, 11, 0, 4, 1, 15, 6, 14, 10, 2, 5],
    [9, 10, 6, 11, 13, 12, 5, 0, 4, 1, 15, 3, 14, 7, 2, 8],
]
HALO = 32


def split(value):
    high = value.astype(jnp.bfloat16)
    low = (value - high.astype(jnp.float32)).astype(jnp.bfloat16)
    return high, low


def np_split(value):
    value = value.astype(np.float32)
    high = value.astype(jnp.bfloat16)
    low = (value - high.astype(np.float32)).astype(jnp.bfloat16)
    return high, low


def radix4_tables(width):
    quarter = width // 4
    k = np.arange(quarter)[:, None]
    m = np.arange(quarter)[None, :]
    blocks = []
    for r in range(4):
        angle = ((4 * k + r) * m % width) * (2.0 * math.pi / width)
        cosine = np.cos(angle) / math.sqrt(width)
        sine = np.sin(angle) / math.sqrt(width)
        blocks.append(np.block([[cosine, sine], [-sine, cosine]]))
    return np_split(np.stack(blocks))


def resampler_tables():
    parts = []
    for j in range(UP):
        sample = np.arange(LANES)[None, :] + LANES * j
        start = 128 * (min(j, 3) - 1)
        column = np.arange(2 * LANES)[:, None] + start
        lag = DOWN * sample // UP - column
        phase = PHASES * (DOWN * sample % UP) // UP
        offset = lag + phase / PHASES - (RT // 2 - 1)
        window = 0.5 + 0.5 * np.cos(math.pi * offset / (RT / 2.0))
        coeff = 0.9 * np.sinc(0.9 * offset) * window
        parts.append(np_split(np.where((lag >= 0) & (lag < RT), coeff, 0.0)))
    out = [np.concatenate([high, low], axis=1) for high, low in parts[:3]]
    out.append(np.concatenate([parts[3][0], parts[4][0]], axis=1))
    out.append(np.concatenate([parts[3][1], parts[4][1]], axis=1))
    return np.stack(out)


def pitched(rows):
    return (rows // SUB // 2 * 2 + 1) * SUB if rows // SUB % 2 == 0 else rows


def lane_iota():
    return lax.broadcasted_iota(jnp.int32, (SUB, LANES), 1)


def prep_kernel(order, blocks, x_ref, o_ref, buf_ref, sems):
    sub, _, length, _ = x_ref.shape
    lane = lane_iota()
    copies = [
        pltpu.make_async_copy(x_ref.at[:, r], buf_ref.at[r, :, 0:length], sems.at[r]) for r in range(4)
    ]
    for copy in copies:
        copy.start()
    for r in range(4):
        copies[r].wait()
        pitch = buf_ref.shape[2]
        flat_ref = buf_ref.at[r].reshape(sub * pitch, LANES)
        for place, dev in enumerate(order):
            for lb in range(blocks):
                for part in range(2):
                    t = (r * blocks + lb) * 2 + part
                    row = 2 * (blocks * dev + lb) + part
                    o_ref[place, t * SUB : (t + 1) * SUB, :] = flat_ref[
                        pl.ds(row, SUB, stride=pitch), :
                    ]
    for place, dev in enumerate(order):
        for part in range(2):
            total = jnp.zeros((SUB, LANES), jnp.float32)
            if dev > 0:
                last = order.index(dev - 1)
                for r in range(4):
                    t = (r * blocks + blocks - 1) * 2 + part
                    value = o_ref[last, t * SUB : (t + 1) * SUB, :]
                    if r < 3:
                        value = pltpu.roll(value, HALO * (r + 1), 1)
                    total = jnp.where(lane // HALO == r, value, total)
            t = 8 * blocks + part
            o_ref[place, t * SUB : (t + 1) * SUB, :] = total


def main_kernel(
    inputs, order, frames, x_ref, w_hi, w_lo, res_ref, st_ref, at_ref, o_ref,
    a_ref, v_ref, y_ref, yh_ref, yl_ref, z_ref, u_ref, bh_ref, bl_ref,
):
    blocks = frames // LANES
    count = len(inputs)
    place_of = {dev: place for place, dev in enumerate(inputs)}
    f32 = jnp.float32

    def dot(a, b):
        return lax.dot_general(a, b, (((1,), (0,)), ((), ())), preferred_element_type=f32)

    def dot_t(a, b):
        return lax.dot_general(a, b, (((1,), (1,)), ((), ())), preferred_element_type=f32)

    def tile(t):
        return jnp.concatenate(
            [x_ref[place_of[s], t * SUB : (t + 1) * SUB, :] for s in range(count)], axis=0
        )

    halo = [tile(8 * blocks + part).T for part in range(2)]
    for r in range(4):
        rows = [jnp.concatenate([h[r * HALO : (r + 1) * HALO] for h in halo], axis=1)]
        for lb in range(blocks):
            rows.append(
                jnp.concatenate([tile((r * blocks + lb) * 2 + part).T for part in range(2)], axis=1)
            )
        high, low = split(jnp.concatenate(rows, axis=0))
        a_ref[r] = dot(high, w_hi[r]) + dot(low, w_hi[r]) + dot(high, w_lo[r])

    total = frames + HALO

    @pl.loop(0, total // 16, unroll=3)
    def _(i):
        row = pl.ds(pl.multiple_of(i * 16, 16), 16)
        re = [a_ref[r, row, :LANES] for r in range(4)]
        im = [a_ref[r, row, LANES:] for r in range(4)]
        sr, dr = re[0] + re[2], re[0] - re[2]
        si, di = im[0] + im[2], im[0] - im[2]
        tr, er = re[1] + re[3], re[1] - re[3]
        ti, ei = im[1] + im[3], im[1] - im[3]
        v_ref[0, row, :] = sr + tr
        v_ref[4, row, :] = si + ti
        v_ref[1, row, :] = dr - ei
        v_ref[5, row, :] = di + er
        v_ref[2, row, :] = sr - tr
        v_ref[6, row, :] = si - ti
        v_ref[3, row, :] = dr + ei
        v_ref[7, row, :] = di - er

    for k in range(8):
        v_ref[k, total : total + 16, :] = jnp.zeros((16, LANES), f32)
        y_ref[k * 2, 0:SUB, :] = jnp.zeros((SUB, LANES), f32)
        y_ref[k * 2 + 1, 0:SUB, :] = jnp.zeros((SUB, LANES), f32)
        y_ref[16 + k * 2, 0:SUB, :] = jnp.zeros((SUB, LANES), f32)
        y_ref[16 + k * 2 + 1, 0:SUB, :] = jnp.zeros((SUB, LANES), f32)

    taps_len = st_ref.shape[0]
    groups = (total // 4 - 4 + SUB) // SUB
    for q in range(4):

        def step(t, q=q):
            base = t * 32 + 16
            accs = {}
            vals = {}

            def load(part, j):
                vals[part, j] = v_ref[part * 4 + q, pl.ds(base + j, SUB, stride=4), :]

            for part in range(2):
                for j in range(1, 4):
                    load(part, j)
            for p in range(taps_len):
                tap = jnp.broadcast_to(
                    st_ref[p : p + 1, q * LANES : (q + 1) * LANES], (SUB, LANES)
                )
                for part in range(2):
                    load(part, -p)
                    for b in range(4):
                        term = tap * vals[part, b - p]
                        accs[part, b] = term if p == 0 else accs[part, b] + term
            for part in range(2):
                for b in range(4):
                    row = pl.ds(t * SUB + SUB, SUB) if isinstance(t, int) else pl.ds(pl.multiple_of(t * SUB, SUB) + SUB, SUB)
                    y_ref[part * 16 + b * 4 + q, row, :] = accs[part, b]

        if q >= 2:
            for t in range(groups):
                step(t)
        else:
            pl.loop(0, groups, unroll=3)(step)


    rows = groups * SUB
    both = 2 * rows
    for b in range(4):
        for q in range(4):
            value = jnp.concatenate(
                [y_ref[part * 16 + b * 4 + q, SUB : SUB + rows, :] for part in range(2)], axis=0
            )
            high, low = split(value)
            first = b * both + (both if q == 3 else 0)
            yh_ref[q, first : first + both, :] = high
            yl_ref[q, first : first + both, :] = low
    value = jnp.concatenate(
        [y_ref[part * 16 + 15, SUB - 1 : SUB - 1 + rows, :] for part in range(2)], axis=0
    )
    high, low = split(value)
    yh_ref[3, 0:both, :] = high
    yl_ref[3, 0:both, :] = low

    def store_z(j, value):
        for b in range(4):
            g, q = (5 * b + j) // 4, (5 * b + j) % 4
            for part in range(2):
                first = b * both + part * rows
                z_ref[part * 20 + g * 4 + q] = value[first : first + rows]

    def pair(ref, left, right):
        first = both if left == 2 else 0
        a = ref[3, 0 : 4 * both] if left < 0 else ref[left, 0 : 4 * both]
        return jnp.concatenate([a, ref[right, first if right == 3 else 0 : (first if right == 3 else 0) + 4 * both]], axis=1)

    for j in range(3):
        high = pair(yh_ref, j - 1, j)
        low = pair(yl_ref, j - 1, j)
        wide = dot(high, res_ref[j])
        store_z(j, wide[:, :LANES] + wide[:, LANES:] + dot(low, res_ref[j, :, :LANES]))
    high = pair(yh_ref, 2, 3)
    low = pair(yl_ref, 2, 3)
    wide = dot(high, res_ref[3]) + dot(high, res_ref[4]) + dot(low, res_ref[3])
    store_z(3, wide[:, :LANES])
    store_z(4, wide[:, LANES:])

    outs = frames * UP // DOWN
    taps_len = at_ref.shape[0]
    groups2 = frames // 4 // SUB
    for q in range(4):

        def step(t, q=q):
            accs = {}
            vals = {}

            def load(part, j):
                shift = j // UP
                slot = part * 20 + (j - UP * shift) * 4 + q
                vals[part, j] = z_ref[slot, pl.ds(t * SUB + 4 + shift, SUB), :]

            for part in range(2):
                for j in range(1, UP):
                    load(part, j)
            for p in range(taps_len):
                tap = jnp.broadcast_to(
                    at_ref[p : p + 1, q * LANES : (q + 1) * LANES], (SUB, LANES)
                )
                for part in range(2):
                    load(part, -p)
                    for g in range(UP):
                        term = tap * vals[part, g - p]
                        accs[part, g] = term if p == 0 else accs[part, g] + term
            for part in range(2):
                for g in range(UP):
                    row = pl.ds(t * SUB * UP + g, SUB, stride=UP)
                    u_ref[part * 4 + q, row, :] = accs[part, g]

        if q == 0:
            for t in range(groups2):
                step(t)
        else:
            pl.loop(0, groups2, unroll=4)(step)


    @pl.loop(0, outs // 16, unroll=4)
    def _(i):
        row = pl.ds(pl.multiple_of(i * 16, 16), 16)
        re = [u_ref[q, row, :] for q in range(4)]
        im = [u_ref[4 + q, row, :] for q in range(4)]
        sr, dr = re[0] + re[2], re[0] - re[2]
        si, di = im[0] + im[2], im[0] - im[2]
        tr, er = re[1] + re[3], re[1] - re[3]
        ti, ei = im[1] + im[3], im[1] - im[3]
        spectra = [
            (sr + tr, si + ti), (dr + ei, di - er), (sr - tr, si - ti), (dr - ei, di + er)
        ]
        for r in range(4):
            for part in range(2):
                high, low = split(spectra[r][part])
                cols = slice(part * LANES, (part + 1) * LANES)
                bh_ref[r, row, cols] = high
                bl_ref[r, row, cols] = low

    lane = lax.broadcasted_iota(jnp.int32, (LANES, LANES), 1)
    full = outs // LANES
    rest = outs - full * LANES
    for r in range(4):
        for place in range(2):
            first = full * LANES + place * rest
            last = slice(full * LANES, full * LANES + rest)
            if place == 1:
                bh_ref[r, first : first + rest] = bh_ref[r, last]
            bh_ref[r, first + LANES : first + LANES + rest] = bl_ref[r, last]
        main = slice(0, full * LANES)
        high, low = bh_ref[r, main], bl_ref[r, main]
        out = dot_t(w_hi[r], high) + dot_t(w_hi[r], low) + dot_t(w_lo[r], high)
        tail = dot_t(w_hi[r], bh_ref[r, full * LANES :])
        tail = tail[:, :LANES] + tail[:, LANES:]
        tail = tail + dot_t(w_lo[r], bh_ref[r, full * LANES : (full + 1) * LANES])
        for part in range(2):
            for k in range(full):
                t = k * SUB + r * 2 + part
                value = out[part * LANES : (part + 1) * LANES, k * LANES : (k + 1) * LANES]
                for place, dev in enumerate(order):
                    o_ref[place, t * SUB : (t + 1) * SUB, :] = value[dev * SUB : (dev + 1) * SUB]
        value = jnp.where(lane < rest, tail[:LANES], tail[LANES:])
        t = full * SUB + r
        for place, dev in enumerate(order):
            o_ref[place, t * SUB : (t + 1) * SUB, :] = value[dev * SUB : (dev + 1) * SUB]


def final_kernel(order, x_ref, o_ref, buf_ref, sems):
    _, _, length, _ = o_ref.shape
    lane = lane_iota()
    half = LANES // 2
    place_of = {dev: place for place, dev in enumerate(order)}
    copies = []

    def tile(dev, t):
        return x_ref[place_of[dev], t * SUB : (t + 1) * SUB, :]

    for r in range(4):
        pitch = buf_ref.shape[2]
        flat_ref = buf_ref.at[r].reshape(SUB * pitch, LANES)
        for dev in range(0, len(order), 2):
            for part in range(2):
                t = r * 2 + part
                ends = [tile(dev, 16 + r), tile(dev + 1, 16 + r)]
                ends[1 - part] = pltpu.roll(ends[1 - part], half, 1)
                r0 = pltpu.roll(tile(dev + 1, t), half, 1)
                r1 = pltpu.roll(tile(dev + 1, 8 + t), half, 1)
                values = [
                    tile(dev, t),
                    tile(dev, 8 + t),
                    jnp.where(lane < half, ends[0], r0),
                    jnp.where(lane < half, r0, r1),
                    jnp.where(lane < half, r1, ends[1]),
                ]
                for k, value in enumerate(values):
                    first = (5 * (dev // 2) + k) * 2 + part
                    flat_ref[pl.ds(first, SUB, stride=pitch), :] = value
        copies.append(pltpu.make_async_copy(buf_ref.at[r, :, 0:length], o_ref.at[:, r], sems.at[r]))
        copies[-1].start()
    for copy in copies:
        copy.wait()


def shards(order_in, order_out, spectra, synth_taps, analysis_taps):
    count = lax.axis_size("tm")
    channels, parts, length = spectra.shape
    width = channels * count
    frames = length // count
    outs = frames * UP // DOWN
    blocks = frames // LANES
    tiled = channels == 4 * SUB
    vmem = pl.BlockSpec(memory_space=pltpu.VMEM)
    hbm = pl.BlockSpec(memory_space=pltpu.HBM)
    f32, bf16 = jnp.float32, jnp.bfloat16
    rows_in = 8 * blocks * SUB + 2 * SUB
    rows_out = (outs * 64) // LANES
    sub = channels // 4
    small = pltpu.CompilerParams(vmem_limit_bytes=8 << 20)

    def exchange(value, order):
        return lax.all_to_all(
            value, "tm", split_axis=0, concat_axis=0, tiled=True, axis_index_groups=[list(order)]
        )

    if tiled:
        flat = spectra.reshape(channels, 2, length // LANES, LANES).transpose(0, 2, 1, 3)
        flat = flat.reshape(sub, 4, -1, LANES)
        flat = pltpu.with_memory_space_constraint(flat, pltpu.HBM)
        sent = pl.pallas_call(
            functools.partial(prep_kernel, order_in, blocks),
            out_shape=jax.ShapeDtypeStruct((count, rows_in, LANES), f32),
            in_specs=[hbm],
            out_specs=vmem,
            scratch_shapes=[
                pltpu.VMEM((4, sub, pitched(flat.shape[2]), LANES), f32),
                pltpu.SemaphoreType.DMA((4,)),
            ],
            compiler_params=small,
        )(flat)
        received = exchange(sent, order_in)
        inner = (order_in, order_out)
    else:
        cut = spectra.reshape(sub, 4, 2, count, blocks, LANES).transpose(3, 1, 4, 2, 0, 5)
        tail = spectra.reshape(sub, 4, 2, count, frames)[..., frames - HALO :]
        tail = jnp.concatenate([jnp.zeros_like(tail[..., :1, :]), tail[..., :-1, :]], axis=3)
        tail = tail.transpose(3, 2, 0, 1, 4).reshape(count, 2 * sub, LANES)
        sent = jnp.concatenate([cut.reshape(count, 8 * blocks * sub, LANES), tail], axis=1)
        received = exchange(sent, range(count))
        tiles = 8 * blocks + 2
        inner = (range(width // 4 // SUB),) * 2
        received = received.reshape(count, tiles, sub, LANES).transpose(1, 0, 2, 3)
        received = received.reshape(tiles, len(inner[0]), SUB, LANES).transpose(1, 0, 2, 3)
        received = received.reshape(len(inner[0]), tiles * SUB, LANES)

    w_hi, w_lo = radix4_tables(width)
    res = resampler_tables()
    rows = ((frames + HALO) // 4 - 4 + SUB) // SUB * SUB
    made = pl.pallas_call(
        functools.partial(main_kernel, *inner, frames),
        out_shape=jax.ShapeDtypeStruct((len(inner[0]), rows_out, LANES), f32),
        in_specs=[vmem] * 6,
        out_specs=vmem,
        scratch_shapes=[
            pltpu.VMEM((4, frames + HALO, 2 * LANES), f32),
            pltpu.VMEM((8, frames + HALO + 16, LANES), f32),
            pltpu.VMEM((32, rows + SUB, LANES), f32),
            pltpu.VMEM((4, 10 * rows, LANES), bf16),
            pltpu.VMEM((4, 10 * rows, LANES), bf16),
            pltpu.VMEM((40, rows, LANES), f32),
            pltpu.VMEM((8, outs, LANES), f32),
            pltpu.VMEM((4, outs + 3 * (outs % LANES), 2 * LANES), bf16),
            pltpu.VMEM((4, outs, 2 * LANES), bf16),
        ],
        compiler_params=pltpu.CompilerParams(vmem_limit_bytes=24 << 20),
    )(received, w_hi, w_lo, res, synth_taps, analysis_taps)

    if tiled:
        back = exchange(made, order_out)
        out = pl.pallas_call(
            functools.partial(final_kernel, order_out),
            out_shape=jax.ShapeDtypeStruct((sub, 4, 2 * count * outs // LANES, LANES), f32),
            in_specs=[vmem],
            out_specs=hbm,
            scratch_shapes=[
                pltpu.VMEM((4, sub, pitched(2 * count * outs // LANES), LANES), f32),
                pltpu.SemaphoreType.DMA((4,)),
            ],
            compiler_params=small,
        )(back)
        out = out.reshape(channels, count * outs // LANES, 2, LANES).transpose(0, 2, 1, 3)
        return out.reshape(channels, 2, count * outs)
    tiles = rows_out // SUB
    made = made.reshape(len(inner[0]), tiles, SUB, LANES).transpose(1, 0, 2, 3)
    made = made.reshape(tiles, count, sub, LANES).transpose(1, 0, 2, 3)
    back = exchange(made, range(count))
    full = outs // LANES
    head = back[:, : 8 * full].reshape(count, full, 4, 2, sub, LANES).transpose(4, 2, 3, 0, 1, 5)
    head = head.reshape(channels, 2, count, full * LANES)
    rest = back[:, 8 * full :].reshape(count, 4, sub, 2, outs - full * LANES).transpose(2, 1, 3, 0, 4)
    rest = rest.reshape(channels, 2, count, -1)
    return jnp.concatenate([head, rest], axis=3).reshape(channels, 2, count * outs)


def solution(mesh):
    in_specs = (P("tm", "station", None), P(), P())
    out_specs = P("tm", "station", None)
    orders = [list(range(mesh.shape["tm"]))] * 2
    if len(orders[0]) == len(ORDERS[0]):
        orders = ORDERS
    return jax.shard_map(
        functools.partial(shards, *orders),
        mesh=mesh,
        in_specs=in_specs,
        out_specs=out_specs,
        check_vma=False,
    )
```

```python
import functools
import math

import jax
import jax.numpy as jnp
import numpy as np
from jax import lax
from jax.experimental import pallas as pl
from jax.experimental.pallas import tpu as pltpu
from jax.sharding import PartitionSpec as P

RT = 32
PHASES = 64
UP, DOWN = 5, 4
LANES = 128
SUB = 8
ORDERS = [
    [9, 3, 7, 13, 12, 8, 11, 0, 4, 1, 15, 6, 14, 10, 2, 5],
    [9, 10, 6, 5, 13, 12, 11, 0, 4, 1, 15, 3, 14, 7, 2, 8],
]
HALO = 32


def split(value):
    high = value.astype(jnp.bfloat16)
    low = (value - high.astype(jnp.float32)).astype(jnp.bfloat16)
    return high, low


def np_split(value):
    value = value.astype(np.float32)
    high = value.astype(jnp.bfloat16)
    low = (value - high.astype(np.float32)).astype(jnp.bfloat16)
    return high, low


def radix4_tables(width):
    quarter = width // 4
    k = np.arange(quarter)[:, None]
    m = np.arange(quarter)[None, :]
    blocks = []
    for r in range(4):
        angle = ((4 * k + r) * m % width) * (2.0 * math.pi / width)
        cosine = np.cos(angle) / math.sqrt(width)
        sine = np.sin(angle) / math.sqrt(width)
        blocks.append(np.block([[cosine, sine], [-sine, cosine]]))
    return np_split(np.stack(blocks))


def resampler_tables():
    parts = []
    for j in range(UP):
        sample = np.arange(LANES)[None, :] + LANES * j
        start = 128 * (min(j, 3) - 1)
        column = np.arange(2 * LANES)[:, None] + start
        lag = DOWN * sample // UP - column
        phase = PHASES * (DOWN * sample % UP) // UP
        offset = lag + phase / PHASES - (RT // 2 - 1)
        window = 0.5 + 0.5 * np.cos(math.pi * offset / (RT / 2.0))
        coeff = 0.9 * np.sinc(0.9 * offset) * window
        parts.append(np_split(np.where((lag >= 0) & (lag < RT), coeff, 0.0)))
    out = [np.concatenate([high, low], axis=1) for high, low in parts[:3]]
    out.append(np.concatenate([parts[3][0], parts[4][0]], axis=1))
    out.append(np.concatenate([parts[3][1], parts[4][1]], axis=1))
    return np.stack(out)


def pitched(rows):
    return (rows // SUB // 2 * 2 + 1) * SUB if rows // SUB % 2 == 0 else rows


def lane_iota():
    return lax.broadcasted_iota(jnp.int32, (SUB, LANES), 1)


def prep_kernel(order, blocks, x_ref, o_ref, buf_ref, sems):
    sub, _, length, _ = x_ref.shape
    lane = lane_iota()
    copies = [
        pltpu.make_async_copy(x_ref.at[:, r], buf_ref.at[r, :, 0:length], sems.at[r]) for r in range(4)
    ]
    for copy in copies:
        copy.start()
    for r in range(4):
        copies[r].wait()
        pitch = buf_ref.shape[2]
        flat_ref = buf_ref.at[r].reshape(sub * pitch, LANES)
        for place, dev in enumerate(order):
            for lb in range(blocks):
                for part in range(2):
                    t = (r * blocks + lb) * 2 + part
                    row = 2 * (blocks * dev + lb) + part
                    o_ref[place, t * SUB : (t + 1) * SUB, :] = flat_ref[
                        pl.ds(row, SUB, stride=pitch), :
                    ]
    for place, dev in enumerate(order):
        for part in range(2):
            total = jnp.zeros((SUB, LANES), jnp.float32)
            if dev > 0:
                last = order.index(dev - 1)
                for r in range(4):
                    t = (r * blocks + blocks - 1) * 2 + part
                    value = o_ref[last, t * SUB : (t + 1) * SUB, :]
                    if r < 3:
                        value = pltpu.roll(value, HALO * (r + 1), 1)
                    total = jnp.where(lane // HALO == r, value, total)
            t = 8 * blocks + part
            o_ref[place, t * SUB : (t + 1) * SUB, :] = total


def main_kernel(
    inputs, order, frames, x_ref, w_hi, w_lo, res_ref, st_ref, at_ref, o_ref,
    a_ref, v_ref, y_ref, yh_ref, yl_ref, z_ref, u_ref, bh_ref, bl_ref,
):
    blocks = frames // LANES
    count = len(inputs)
    place_of = {dev: place for place, dev in enumerate(inputs)}
    f32 = jnp.float32

    def dot(a, b):
        return lax.dot_general(a, b, (((1,), (0,)), ((), ())), preferred_element_type=f32)

    def dot_t(a, b):
        return lax.dot_general(a, b, (((1,), (1,)), ((), ())), preferred_element_type=f32)

    def tile(t):
        return jnp.concatenate(
            [x_ref[place_of[s], t * SUB : (t + 1) * SUB, :] for s in range(count)], axis=0
        )

    halo = [tile(8 * blocks + part).T for part in range(2)]
    for r in range(4):
        rows = [jnp.concatenate([h[r * HALO : (r + 1) * HALO] for h in halo], axis=1)]
        for lb in range(blocks):
            rows.append(
                jnp.concatenate([tile((r * blocks + lb) * 2 + part).T for part in range(2)], axis=1)
            )
        high, low = split(jnp.concatenate(rows, axis=0))
        a_ref[r] = dot(high, w_hi[r]) + dot(low, w_hi[r]) + dot(high, w_lo[r])

    total = frames + HALO

    @pl.loop(0, total // 16, unroll=3)
    def _(i):
        row = pl.ds(pl.multiple_of(i * 16, 16), 16)
        re = [a_ref[r, row, :LANES] for r in range(4)]
        im = [a_ref[r, row, LANES:] for r in range(4)]
        sr, dr = re[0] + re[2], re[0] - re[2]
        si, di = im[0] + im[2], im[0] - im[2]
        tr, er = re[1] + re[3], re[1] - re[3]
        ti, ei = im[1] + im[3], im[1] - im[3]
        v_ref[0, row, :] = sr + tr
        v_ref[4, row, :] = si + ti
        v_ref[1, row, :] = dr - ei
        v_ref[5, row, :] = di + er
        v_ref[2, row, :] = sr - tr
        v_ref[6, row, :] = si - ti
        v_ref[3, row, :] = dr + ei
        v_ref[7, row, :] = di - er

    for k in range(8):
        v_ref[k, total : total + 16, :] = jnp.zeros((16, LANES), f32)
        y_ref[k * 2, 0:SUB, :] = jnp.zeros((SUB, LANES), f32)
        y_ref[k * 2 + 1, 0:SUB, :] = jnp.zeros((SUB, LANES), f32)
        y_ref[16 + k * 2, 0:SUB, :] = jnp.zeros((SUB, LANES), f32)
        y_ref[16 + k * 2 + 1, 0:SUB, :] = jnp.zeros((SUB, LANES), f32)

    taps_len = st_ref.shape[0]
    groups = (total // 4 - 4 + SUB) // SUB
    for q in range(4):

        def step(t, q=q):
            base = t * 32 + 16
            accs = {}
            vals = {}

            def load(part, j):
                vals[part, j] = v_ref[part * 4 + q, pl.ds(base + j, SUB, stride=4), :]

            for part in range(2):
                for j in range(1, 4):
                    load(part, j)
            for p in range(taps_len):
                tap = jnp.broadcast_to(
                    st_ref[p : p + 1, q * LANES : (q + 1) * LANES], (SUB, LANES)
                )
                for part in range(2):
                    load(part, -p)
                    for b in range(4):
                        term = tap * vals[part, b - p]
                        accs[part, b] = term if p == 0 else accs[part, b] + term
            for part in range(2):
                for b in range(4):
                    row = pl.ds(t * SUB + SUB, SUB) if isinstance(t, int) else pl.ds(pl.multiple_of(t * SUB, SUB) + SUB, SUB)
                    y_ref[part * 16 + b * 4 + q, row, :] = accs[part, b]

        if q >= 2:
            for t in range(groups):
                step(t)
        else:
            pl.loop(0, groups, unroll=3)(step)


    rows = groups * SUB
    both = 2 * rows
    for b in range(4):
        for q in range(4):
            value = jnp.concatenate(
                [y_ref[part * 16 + b * 4 + q, SUB : SUB + rows, :] for part in range(2)], axis=0
            )
            high, low = split(value)
            first = b * both + (both if q == 3 else 0)
            yh_ref[q, first : first + both, :] = high
            yl_ref[q, first : first + both, :] = low
    value = jnp.concatenate(
        [y_ref[part * 16 + 15, SUB - 1 : SUB - 1 + rows, :] for part in range(2)], axis=0
    )
    high, low = split(value)
    yh_ref[3, 0:both, :] = high
    yl_ref[3, 0:both, :] = low

    def store_z(j, value):
        for b in range(4):
            g, q = (5 * b + j) // 4, (5 * b + j) % 4
            for part in range(2):
                first = b * both + part * rows
                z_ref[part * 20 + g * 4 + q] = value[first : first + rows]

    def pair(ref, left, right):
        first = both if left == 2 else 0
        a = ref[3, 0 : 4 * both] if left < 0 else ref[left, 0 : 4 * both]
        return jnp.concatenate([a, ref[right, first if right == 3 else 0 : (first if right == 3 else 0) + 4 * both]], axis=1)

    for j in range(3):
        high = pair(yh_ref, j - 1, j)
        low = pair(yl_ref, j - 1, j)
        wide = dot(high, res_ref[j])
        store_z(j, wide[:, :LANES] + wide[:, LANES:] + dot(low, res_ref[j, :, :LANES]))
    high = pair(yh_ref, 2, 3)
    low = pair(yl_ref, 2, 3)
    wide = dot(high, res_ref[3]) + dot(high, res_ref[4]) + dot(low, res_ref[3])
    store_z(3, wide[:, :LANES])
    store_z(4, wide[:, LANES:])

    outs = frames * UP // DOWN
    taps_len = at_ref.shape[0]
    groups2 = frames // 4 // SUB
    for q in range(4):

        def step(t, q=q):
            accs = {}
            vals = {}

            def load(part, j):
                shift = j // UP
                slot = part * 20 + (j - UP * shift) * 4 + q
                vals[part, j] = z_ref[slot, pl.ds(t * SUB + 4 + shift, SUB), :]

            for part in range(2):
                for j in range(1, UP):
                    load(part, j)
            for p in range(taps_len):
                tap = jnp.broadcast_to(
                    at_ref[p : p + 1, q * LANES : (q + 1) * LANES], (SUB, LANES)
                )
                for part in range(2):
                    load(part, -p)
                    for g in range(UP):
                        term = tap * vals[part, g - p]
                        accs[part, g] = term if p == 0 else accs[part, g] + term
            for part in range(2):
                for g in range(UP):
                    row = pl.ds(t * SUB * UP + g, SUB, stride=UP)
                    u_ref[part * 4 + q, row, :] = accs[part, g]

        if q == 0:
            for t in range(groups2):
                step(t)
        else:
            pl.loop(0, groups2, unroll=4)(step)


    @pl.loop(0, outs // 16, unroll=4)
    def _(i):
        row = pl.ds(pl.multiple_of(i * 16, 16), 16)
        re = [u_ref[q, row, :] for q in range(4)]
        im = [u_ref[4 + q, row, :] for q in range(4)]
        sr, dr = re[0] + re[2], re[0] - re[2]
        si, di = im[0] + im[2], im[0] - im[2]
        tr, er = re[1] + re[3], re[1] - re[3]
        ti, ei = im[1] + im[3], im[1] - im[3]
        spectra = [
            (sr + tr, si + ti), (dr + ei, di - er), (sr - tr, si - ti), (dr - ei, di + er)
        ]
        for r in range(4):
            for part in range(2):
                high, low = split(spectra[r][part])
                cols = slice(part * LANES, (part + 1) * LANES)
                bh_ref[r, row, cols] = high
                bl_ref[r, row, cols] = low

    lane = lax.broadcasted_iota(jnp.int32, (LANES, LANES), 1)
    full = outs // LANES
    rest = outs - full * LANES
    for r in range(4):
        for place in range(2):
            first = full * LANES + place * rest
            last = slice(full * LANES, full * LANES + rest)
            if place == 1:
                bh_ref[r, first : first + rest] = bh_ref[r, last]
            bh_ref[r, first + LANES : first + LANES + rest] = bl_ref[r, last]
        main = slice(0, full * LANES)
        high, low = bh_ref[r, main], bl_ref[r, main]
        out = dot_t(w_hi[r], high) + dot_t(w_hi[r], low) + dot_t(w_lo[r], high)
        tail = dot_t(w_hi[r], bh_ref[r, full * LANES :])
        tail = tail[:, :LANES] + tail[:, LANES:]
        tail = tail + dot_t(w_lo[r], bh_ref[r, full * LANES : (full + 1) * LANES])
        for part in range(2):
            for k in range(full):
                t = k * SUB + r * 2 + part
                value = out[part * LANES : (part + 1) * LANES, k * LANES : (k + 1) * LANES]
                for place, dev in enumerate(order):
                    o_ref[place, t * SUB : (t + 1) * SUB, :] = value[dev * SUB : (dev + 1) * SUB]
        value = jnp.where(lane < rest, tail[:LANES], tail[LANES:])
        t = full * SUB + r
        for place, dev in enumerate(order):
            o_ref[place, t * SUB : (t + 1) * SUB, :] = value[dev * SUB : (dev + 1) * SUB]


def final_kernel(order, x_ref, o_ref, buf_ref, sems):
    _, _, length, _ = o_ref.shape
    lane = lane_iota()
    half = LANES // 2
    place_of = {dev: place for place, dev in enumerate(order)}
    copies = []

    def tile(dev, t):
        return x_ref[place_of[dev], t * SUB : (t + 1) * SUB, :]

    for r in range(4):
        pitch = buf_ref.shape[2]
        flat_ref = buf_ref.at[r].reshape(SUB * pitch, LANES)
        for dev in range(0, len(order), 2):
            for part in range(2):
                t = r * 2 + part
                ends = [tile(dev, 16 + r), tile(dev + 1, 16 + r)]
                ends[1 - part] = pltpu.roll(ends[1 - part], half, 1)
                r0 = pltpu.roll(tile(dev + 1, t), half, 1)
                r1 = pltpu.roll(tile(dev + 1, 8 + t), half, 1)
                values = [
                    tile(dev, t),
                    tile(dev, 8 + t),
                    jnp.where(lane < half, ends[0], r0),
                    jnp.where(lane < half, r0, r1),
                    jnp.where(lane < half, r1, ends[1]),
                ]
                for k, value in enumerate(values):
                    first = (5 * (dev // 2) + k) * 2 + part
                    flat_ref[pl.ds(first, SUB, stride=pitch), :] = value
        copies.append(pltpu.make_async_copy(buf_ref.at[r, :, 0:length], o_ref.at[:, r], sems.at[r]))
        copies[-1].start()
    for copy in copies:
        copy.wait()


def shards(order_in, order_out, spectra, synth_taps, analysis_taps):
    count = lax.axis_size("tm")
    channels, parts, length = spectra.shape
    width = channels * count
    frames = length // count
    outs = frames * UP // DOWN
    blocks = frames // LANES
    tiled = channels == 4 * SUB
    vmem = pl.BlockSpec(memory_space=pltpu.VMEM)
    hbm = pl.BlockSpec(memory_space=pltpu.HBM)
    f32, bf16 = jnp.float32, jnp.bfloat16
    rows_in = 8 * blocks * SUB + 2 * SUB
    rows_out = (outs * 64) // LANES
    sub = channels // 4
    small = pltpu.CompilerParams(vmem_limit_bytes=8 << 20)

    def exchange(value, order):
        return lax.all_to_all(
            value, "tm", split_axis=0, concat_axis=0, tiled=True, axis_index_groups=[list(order)]
        )

    if tiled:
        flat = spectra.reshape(channels, 2, length // LANES, LANES).transpose(0, 2, 1, 3)
        flat = flat.reshape(sub, 4, -1, LANES)
        flat = pltpu.with_memory_space_constraint(flat, pltpu.HBM)
        sent = pl.pallas_call(
            functools.partial(prep_kernel, order_in, blocks),
            out_shape=jax.ShapeDtypeStruct((count, rows_in, LANES), f32),
            in_specs=[hbm],
            out_specs=vmem,
            scratch_shapes=[
                pltpu.VMEM((4, sub, pitched(flat.shape[2]), LANES), f32),
                pltpu.SemaphoreType.DMA((4,)),
            ],
            compiler_params=small,
        )(flat)
        received = exchange(sent, order_in)
        inner = (order_in, order_out)
    else:
        cut = spectra.reshape(sub, 4, 2, count, blocks, LANES).transpose(3, 1, 4, 2, 0, 5)
        tail = spectra.reshape(sub, 4, 2, count, frames)[..., frames - HALO :]
        tail = jnp.concatenate([jnp.zeros_like(tail[..., :1, :]), tail[..., :-1, :]], axis=3)
        tail = tail.transpose(3, 2, 0, 1, 4).reshape(count, 2 * sub, LANES)
        sent = jnp.concatenate([cut.reshape(count, 8 * blocks * sub, LANES), tail], axis=1)
        received = exchange(sent, range(count))
        tiles = 8 * blocks + 2
        inner = (range(width // 4 // SUB),) * 2
        received = received.reshape(count, tiles, sub, LANES).transpose(1, 0, 2, 3)
        received = received.reshape(tiles, len(inner[0]), SUB, LANES).transpose(1, 0, 2, 3)
        received = received.reshape(len(inner[0]), tiles * SUB, LANES)

    w_hi, w_lo = radix4_tables(width)
    res = resampler_tables()
    rows = ((frames + HALO) // 4 - 4 + SUB) // SUB * SUB
    made = pl.pallas_call(
        functools.partial(main_kernel, *inner, frames),
        out_shape=jax.ShapeDtypeStruct((len(inner[0]), rows_out, LANES), f32),
        in_specs=[vmem] * 6,
        out_specs=vmem,
        scratch_shapes=[
            pltpu.VMEM((4, frames + HALO, 2 * LANES), f32),
            pltpu.VMEM((8, frames + HALO + 16, LANES), f32),
            pltpu.VMEM((32, rows + SUB, LANES), f32),
            pltpu.VMEM((4, 10 * rows, LANES), bf16),
            pltpu.VMEM((4, 10 * rows, LANES), bf16),
            pltpu.VMEM((40, rows, LANES), f32),
            pltpu.VMEM((8, outs, LANES), f32),
            pltpu.VMEM((4, outs + 3 * (outs % LANES), 2 * LANES), bf16),
            pltpu.VMEM((4, outs, 2 * LANES), bf16),
        ],
        compiler_params=pltpu.CompilerParams(vmem_limit_bytes=24 << 20),
    )(received, w_hi, w_lo, res, synth_taps, analysis_taps)

    if tiled:
        back = exchange(made, order_out)
        out = pl.pallas_call(
            functools.partial(final_kernel, order_out),
            out_shape=jax.ShapeDtypeStruct((sub, 4, 2 * count * outs // LANES, LANES), f32),
            in_specs=[vmem],
            out_specs=hbm,
            scratch_shapes=[
                pltpu.VMEM((4, sub, pitched(2 * count * outs // LANES), LANES), f32),
                pltpu.SemaphoreType.DMA((4,)),
            ],
            compiler_params=small,
        )(back)
        out = out.reshape(channels, count * outs // LANES, 2, LANES).transpose(0, 2, 1, 3)
        return out.reshape(channels, 2, count * outs)
    tiles = rows_out // SUB
    made = made.reshape(len(inner[0]), tiles, SUB, LANES).transpose(1, 0, 2, 3)
    made = made.reshape(tiles, count, sub, LANES).transpose(1, 0, 2, 3)
    back = exchange(made, range(count))
    full = outs // LANES
    head = back[:, : 8 * full].reshape(count, full, 4, 2, sub, LANES).transpose(4, 2, 3, 0, 1, 5)
    head = head.reshape(channels, 2, count, full * LANES)
    rest = back[:, 8 * full :].reshape(count, 4, sub, 2, outs - full * LANES).transpose(2, 1, 3, 0, 4)
    rest = rest.reshape(channels, 2, count, -1)
    return jnp.concatenate([head, rest], axis=3).reshape(channels, 2, count * outs)


def solution(mesh):
    in_specs = (P("tm", "station", None), P(), P())
    out_specs = P("tm", "station", None)
    orders = [list(range(mesh.shape["tm"]))] * 2
    if len(orders[0]) == len(ORDERS[0]):
        orders = ORDERS
    return jax.shard_map(
        functools.partial(shards, *orders),
        mesh=mesh,
        in_specs=in_specs,
        out_specs=out_specs,
        check_vma=False,
    )
```

```python
import functools
import math

import jax
import jax.numpy as jnp
import numpy as np
from jax import lax
from jax.experimental import pallas as pl
from jax.experimental.pallas import tpu as pltpu
from jax.sharding import PartitionSpec as P

RT = 32
PHASES = 64
UP, DOWN = 5, 4
LANES = 128
SUB = 8
ORDERS = [
    [9, 3, 7, 13, 12, 8, 11, 0, 4, 1, 15, 6, 14, 10, 2, 5],
    [9, 10, 6, 5, 13, 12, 11, 0, 4, 1, 15, 3, 14, 7, 2, 8],
]
HALO = 32


def split(value):
    high = value.astype(jnp.bfloat16)
    low = (value - high.astype(jnp.float32)).astype(jnp.bfloat16)
    return high, low


def np_split(value):
    value = value.astype(np.float32)
    high = value.astype(jnp.bfloat16)
    low = (value - high.astype(np.float32)).astype(jnp.bfloat16)
    return high, low


def radix4_tables(width):
    quarter = width // 4
    k = np.arange(quarter)[:, None]
    m = np.arange(quarter)[None, :]
    blocks = []
    for r in range(4):
        angle = ((4 * k + r) * m % width) * (2.0 * math.pi / width)
        cosine = np.cos(angle) / math.sqrt(width)
        sine = np.sin(angle) / math.sqrt(width)
        blocks.append(np.block([[cosine, sine], [-sine, cosine]]))
    return np_split(np.stack(blocks))


def resampler_tables():
    parts = []
    for j in range(UP):
        sample = np.arange(LANES)[None, :] + LANES * j
        start = 128 * (min(j, 3) - 1)
        column = np.arange(2 * LANES)[:, None] + start
        lag = DOWN * sample // UP - column
        phase = PHASES * (DOWN * sample % UP) // UP
        offset = lag + phase / PHASES - (RT // 2 - 1)
        window = 0.5 + 0.5 * np.cos(math.pi * offset / (RT / 2.0))
        coeff = 0.9 * np.sinc(0.9 * offset) * window
        parts.append(np_split(np.where((lag >= 0) & (lag < RT), coeff, 0.0)))
    out = [np.concatenate([high, low], axis=1) for high, low in parts[:3]]
    out.append(np.concatenate([parts[3][0], parts[4][0]], axis=1))
    out.append(np.concatenate([parts[3][1], parts[4][1]], axis=1))
    return np.stack(out)


def pitched(rows):
    return (rows // SUB // 2 * 2 + 1) * SUB if rows // SUB % 2 == 0 else rows


def lane_iota():
    return lax.broadcasted_iota(jnp.int32, (SUB, LANES), 1)


def prep_kernel(order, blocks, x_ref, o_ref, buf_ref, sems):
    sub, _, length, _ = x_ref.shape
    lane = lane_iota()
    copies = [
        pltpu.make_async_copy(x_ref.at[:, r], buf_ref.at[r, :, 0:length], sems.at[r]) for r in range(4)
    ]
    for copy in copies:
        copy.start()
    for r in range(4):
        copies[r].wait()
        pitch = buf_ref.shape[2]
        flat_ref = buf_ref.at[r].reshape(sub * pitch, LANES)
        for place, dev in enumerate(order):
            for lb in range(blocks):
                for part in range(2):
                    t = (r * blocks + lb) * 2 + part
                    row = 2 * (blocks * dev + lb) + part
                    o_ref[place, t * SUB : (t + 1) * SUB, :] = flat_ref[
                        pl.ds(row, SUB, stride=pitch), :
                    ]
    for place, dev in enumerate(order):
        for part in range(2):
            total = jnp.zeros((SUB, LANES), jnp.float32)
            if dev > 0:
                last = order.index(dev - 1)
                for r in range(4):
                    t = (r * blocks + blocks - 1) * 2 + part
                    value = o_ref[last, t * SUB : (t + 1) * SUB, :]
                    if r < 3:
                        value = pltpu.roll(value, HALO * (r + 1), 1)
                    total = jnp.where(lane // HALO == r, value, total)
            t = 8 * blocks + part
            o_ref[place, t * SUB : (t + 1) * SUB, :] = total


def main_kernel(
    inputs, order, frames, x_ref, w_hi, w_lo, res_ref, st_ref, at_ref, o_ref,
    a_ref, v_ref, y_ref, yh_ref, yl_ref, z_ref, u_ref, bh_ref, bl_ref,
):
    blocks = frames // LANES
    count = len(inputs)
    place_of = {dev: place for place, dev in enumerate(inputs)}
    f32 = jnp.float32

    def dot(a, b):
        return lax.dot_general(a, b, (((1,), (0,)), ((), ())), preferred_element_type=f32)

    def dot_t(a, b):
        return lax.dot_general(a, b, (((1,), (1,)), ((), ())), preferred_element_type=f32)

    def tile(t):
        return jnp.concatenate(
            [x_ref[place_of[s], t * SUB : (t + 1) * SUB, :] for s in range(count)], axis=0
        )

    halo = [tile(8 * blocks + part).T for part in range(2)]
    for r in range(4):
        rows = [jnp.concatenate([h[r * HALO : (r + 1) * HALO] for h in halo], axis=1)]
        for lb in range(blocks):
            rows.append(
                jnp.concatenate([tile((r * blocks + lb) * 2 + part).T for part in range(2)], axis=1)
            )
        high, low = split(jnp.concatenate(rows, axis=0))
        a_ref[r] = dot(high, w_hi[r]) + dot(low, w_hi[r]) + dot(high, w_lo[r])

    total = frames + HALO

    @pl.loop(0, total // 16, unroll=3)
    def _(i):
        row = pl.ds(pl.multiple_of(i * 16, 16), 16)
        re = [a_ref[r, row, :LANES] for r in range(4)]
        im = [a_ref[r, row, LANES:] for r in range(4)]
        sr, dr = re[0] + re[2], re[0] - re[2]
        si, di = im[0] + im[2], im[0] - im[2]
        tr, er = re[1] + re[3], re[1] - re[3]
        ti, ei = im[1] + im[3], im[1] - im[3]
        v_ref[0, row, :] = sr + tr
        v_ref[4, row, :] = si + ti
        v_ref[1, row, :] = dr - ei
        v_ref[5, row, :] = di + er
        v_ref[2, row, :] = sr - tr
        v_ref[6, row, :] = si - ti
        v_ref[3, row, :] = dr + ei
        v_ref[7, row, :] = di - er

    for k in range(8):
        v_ref[k, total : total + 16, :] = jnp.zeros((16, LANES), f32)
        y_ref[k * 2, 0:SUB, :] = jnp.zeros((SUB, LANES), f32)
        y_ref[k * 2 + 1, 0:SUB, :] = jnp.zeros((SUB, LANES), f32)
        y_ref[16 + k * 2, 0:SUB, :] = jnp.zeros((SUB, LANES), f32)
        y_ref[16 + k * 2 + 1, 0:SUB, :] = jnp.zeros((SUB, LANES), f32)

    taps_len = st_ref.shape[0]
    groups = (total // 4 - 4 + SUB) // SUB
    for q in range(4):

        def step(t, q=q):
            base = t * 32 + 16
            accs = {}
            vals = {}

            def load(part, j):
                vals[part, j] = v_ref[part * 4 + q, pl.ds(base + j, SUB, stride=4), :]

            for part in range(2):
                for j in range(1, 4):
                    load(part, j)
            for p in range(taps_len):
                tap = jnp.broadcast_to(
                    st_ref[p : p + 1, q * LANES : (q + 1) * LANES], (SUB, LANES)
                )
                for part in range(2):
                    load(part, -p)
                    for b in range(4):
                        term = tap * vals[part, b - p]
                        accs[part, b] = term if p == 0 else accs[part, b] + term
            for part in range(2):
                for b in range(4):
                    row = pl.ds(t * SUB + SUB, SUB) if isinstance(t, int) else pl.ds(pl.multiple_of(t * SUB, SUB) + SUB, SUB)
                    y_ref[part * 16 + b * 4 + q, row, :] = accs[part, b]

        if q >= 1:
            for t in range(groups):
                step(t)
        else:
            pl.loop(0, groups, unroll=3)(step)


    rows = groups * SUB
    both = 2 * rows
    for b in range(4):
        for q in range(4):
            value = jnp.concatenate(
                [y_ref[part * 16 + b * 4 + q, SUB : SUB + rows, :] for part in range(2)], axis=0
            )
            high, low = split(value)
            first = b * both + (both if q == 3 else 0)
            yh_ref[q, first : first + both, :] = high
            yl_ref[q, first : first + both, :] = low
    value = jnp.concatenate(
        [y_ref[part * 16 + 15, SUB - 1 : SUB - 1 + rows, :] for part in range(2)], axis=0
    )
    high, low = split(value)
    yh_ref[3, 0:both, :] = high
    yl_ref[3, 0:both, :] = low

    def store_z(j, value):
        for b in range(4):
            g, q = (5 * b + j) // 4, (5 * b + j) % 4
            for part in range(2):
                first = b * both + part * rows
                z_ref[part * 20 + g * 4 + q] = value[first : first + rows]

    def pair(ref, left, right):
        first = both if left == 2 else 0
        a = ref[3, 0 : 4 * both] if left < 0 else ref[left, 0 : 4 * both]
        return jnp.concatenate([a, ref[right, first if right == 3 else 0 : (first if right == 3 else 0) + 4 * both]], axis=1)

    for j in range(3):
        high = pair(yh_ref, j - 1, j)
        low = pair(yl_ref, j - 1, j)
        wide = dot(high, res_ref[j])
        store_z(j, wide[:, :LANES] + wide[:, LANES:] + dot(low, res_ref[j, :, :LANES]))
    high = pair(yh_ref, 2, 3)
    low = pair(yl_ref, 2, 3)
    wide = dot(high, res_ref[3]) + dot(high, res_ref[4]) + dot(low, res_ref[3])
    store_z(3, wide[:, :LANES])
    store_z(4, wide[:, LANES:])

    outs = frames * UP // DOWN
    taps_len = at_ref.shape[0]
    groups2 = frames // 4 // SUB
    for q in range(4):

        def step(t, q=q):
            accs = {}
            vals = {}

            def load(part, j):
                shift = j // UP
                slot = part * 20 + (j - UP * shift) * 4 + q
                vals[part, j] = z_ref[slot, pl.ds(t * SUB + 4 + shift, SUB), :]

            for part in range(2):
                for j in range(1, UP):
                    load(part, j)
            for p in range(taps_len):
                tap = jnp.broadcast_to(
                    at_ref[p : p + 1, q * LANES : (q + 1) * LANES], (SUB, LANES)
                )
                for part in range(2):
                    load(part, -p)
                    for g in range(UP):
                        term = tap * vals[part, g - p]
                        accs[part, g] = term if p == 0 else accs[part, g] + term
            for part in range(2):
                for g in range(UP):
                    row = pl.ds(t * SUB * UP + g, SUB, stride=UP)
                    u_ref[part * 4 + q, row, :] = accs[part, g]

        if q == 0:
            for t in range(groups2):
                step(t)
        else:
            pl.loop(0, groups2, unroll=4)(step)


    @pl.loop(0, outs // 16, unroll=4)
    def _(i):
        row = pl.ds(pl.multiple_of(i * 16, 16), 16)
        re = [u_ref[q, row, :] for q in range(4)]
        im = [u_ref[4 + q, row, :] for q in range(4)]
        sr, dr = re[0] + re[2], re[0] - re[2]
        si, di = im[0] + im[2], im[0] - im[2]
        tr, er = re[1] + re[3], re[1] - re[3]
        ti, ei = im[1] + im[3], im[1] - im[3]
        spectra = [
            (sr + tr, si + ti), (dr + ei, di - er), (sr - tr, si - ti), (dr - ei, di + er)
        ]
        for r in range(4):
            for part in range(2):
                high, low = split(spectra[r][part])
                cols = slice(part * LANES, (part + 1) * LANES)
                bh_ref[r, row, cols] = high
                bl_ref[r, row, cols] = low

    lane = lax.broadcasted_iota(jnp.int32, (LANES, LANES), 1)
    full = outs // LANES
    rest = outs - full * LANES
    for r in range(4):
        for place in range(2):
            first = full * LANES + place * rest
            last = slice(full * LANES, full * LANES + rest)
            if place == 1:
                bh_ref[r, first : first + rest] = bh_ref[r, last]
            bh_ref[r, first + LANES : first + LANES + rest] = bl_ref[r, last]
        main = slice(0, full * LANES)
        high, low = bh_ref[r, main], bl_ref[r, main]
        out = dot_t(w_hi[r], high) + dot_t(w_hi[r], low) + dot_t(w_lo[r], high)
        tail = dot_t(w_hi[r], bh_ref[r, full * LANES :])
        tail = tail[:, :LANES] + tail[:, LANES:]
        tail = tail + dot_t(w_lo[r], bh_ref[r, full * LANES : (full + 1) * LANES])
        for part in range(2):
            for k in range(full):
                t = k * SUB + r * 2 + part
                value = out[part * LANES : (part + 1) * LANES, k * LANES : (k + 1) * LANES]
                for place, dev in enumerate(order):
                    o_ref[place, t * SUB : (t + 1) * SUB, :] = value[dev * SUB : (dev + 1) * SUB]
        value = jnp.where(lane < rest, tail[:LANES], tail[LANES:])
        t = full * SUB + r
        for place, dev in enumerate(order):
            o_ref[place, t * SUB : (t + 1) * SUB, :] = value[dev * SUB : (dev + 1) * SUB]


def final_kernel(order, x_ref, o_ref, buf_ref, sems):
    _, _, length, _ = o_ref.shape
    lane = lane_iota()
    half = LANES // 2
    place_of = {dev: place for place, dev in enumerate(order)}
    copies = []

    def tile(dev, t):
        return x_ref[place_of[dev], t * SUB : (t + 1) * SUB, :]

    for r in range(4):
        pitch = buf_ref.shape[2]
        flat_ref = buf_ref.at[r].reshape(SUB * pitch, LANES)
        for dev in range(0, len(order), 2):
            for part in range(2):
                t = r * 2 + part
                ends = [tile(dev, 16 + r), tile(dev + 1, 16 + r)]
                ends[1 - part] = pltpu.roll(ends[1 - part], half, 1)
                r0 = pltpu.roll(tile(dev + 1, t), half, 1)
                r1 = pltpu.roll(tile(dev + 1, 8 + t), half, 1)
                values = [
                    tile(dev, t),
                    tile(dev, 8 + t),
                    jnp.where(lane < half, ends[0], r0),
                    jnp.where(lane < half, r0, r1),
                    jnp.where(lane < half, r1, ends[1]),
                ]
                for k, value in enumerate(values):
                    first = (5 * (dev // 2) + k) * 2 + part
                    flat_ref[pl.ds(first, SUB, stride=pitch), :] = value
        copies.append(pltpu.make_async_copy(buf_ref.at[r, :, 0:length], o_ref.at[:, r], sems.at[r]))
        copies[-1].start()
    for copy in copies:
        copy.wait()


def shards(order_in, order_out, spectra, synth_taps, analysis_taps):
    count = lax.axis_size("tm")
    channels, parts, length = spectra.shape
    width = channels * count
    frames = length // count
    outs = frames * UP // DOWN
    blocks = frames // LANES
    tiled = channels == 4 * SUB
    vmem = pl.BlockSpec(memory_space=pltpu.VMEM)
    hbm = pl.BlockSpec(memory_space=pltpu.HBM)
    f32, bf16 = jnp.float32, jnp.bfloat16
    rows_in = 8 * blocks * SUB + 2 * SUB
    rows_out = (outs * 64) // LANES
    sub = channels // 4
    small = pltpu.CompilerParams(vmem_limit_bytes=8 << 20)

    def exchange(value, order):
        return lax.all_to_all(
            value, "tm", split_axis=0, concat_axis=0, tiled=True, axis_index_groups=[list(order)]
        )

    if tiled:
        flat = spectra.reshape(channels, 2, length // LANES, LANES).transpose(0, 2, 1, 3)
        flat = flat.reshape(sub, 4, -1, LANES)
        flat = pltpu.with_memory_space_constraint(flat, pltpu.HBM)
        sent = pl.pallas_call(
            functools.partial(prep_kernel, order_in, blocks),
            out_shape=jax.ShapeDtypeStruct((count, rows_in, LANES), f32),
            in_specs=[hbm],
            out_specs=vmem,
            scratch_shapes=[
                pltpu.VMEM((4, sub, pitched(flat.shape[2]), LANES), f32),
                pltpu.SemaphoreType.DMA((4,)),
            ],
            compiler_params=small,
        )(flat)
        received = exchange(sent, order_in)
        inner = (order_in, order_out)
    else:
        cut = spectra.reshape(sub, 4, 2, count, blocks, LANES).transpose(3, 1, 4, 2, 0, 5)
        tail = spectra.reshape(sub, 4, 2, count, frames)[..., frames - HALO :]
        tail = jnp.concatenate([jnp.zeros_like(tail[..., :1, :]), tail[..., :-1, :]], axis=3)
        tail = tail.transpose(3, 2, 0, 1, 4).reshape(count, 2 * sub, LANES)
        sent = jnp.concatenate([cut.reshape(count, 8 * blocks * sub, LANES), tail], axis=1)
        received = exchange(sent, range(count))
        tiles = 8 * blocks + 2
        inner = (range(width // 4 // SUB),) * 2
        received = received.reshape(count, tiles, sub, LANES).transpose(1, 0, 2, 3)
        received = received.reshape(tiles, len(inner[0]), SUB, LANES).transpose(1, 0, 2, 3)
        received = received.reshape(len(inner[0]), tiles * SUB, LANES)

    w_hi, w_lo = radix4_tables(width)
    res = resampler_tables()
    rows = ((frames + HALO) // 4 - 4 + SUB) // SUB * SUB
    made = pl.pallas_call(
        functools.partial(main_kernel, *inner, frames),
        out_shape=jax.ShapeDtypeStruct((len(inner[0]), rows_out, LANES), f32),
        in_specs=[vmem] * 6,
        out_specs=vmem,
        scratch_shapes=[
            pltpu.VMEM((4, frames + HALO, 2 * LANES), f32),
            pltpu.VMEM((8, frames + HALO + 16, LANES), f32),
            pltpu.VMEM((32, rows + SUB, LANES), f32),
            pltpu.VMEM((4, 10 * rows, LANES), bf16),
            pltpu.VMEM((4, 10 * rows, LANES), bf16),
            pltpu.VMEM((40, rows, LANES), f32),
            pltpu.VMEM((8, outs, LANES), f32),
            pltpu.VMEM((4, outs + 3 * (outs % LANES), 2 * LANES), bf16),
            pltpu.VMEM((4, outs, 2 * LANES), bf16),
        ],
        compiler_params=pltpu.CompilerParams(vmem_limit_bytes=24 << 20),
    )(received, w_hi, w_lo, res, synth_taps, analysis_taps)

    if tiled:
        back = exchange(made, order_out)
        out = pl.pallas_call(
            functools.partial(final_kernel, order_out),
            out_shape=jax.ShapeDtypeStruct((sub, 4, 2 * count * outs // LANES, LANES), f32),
            in_specs=[vmem],
            out_specs=hbm,
            scratch_shapes=[
                pltpu.VMEM((4, sub, pitched(2 * count * outs // LANES), LANES), f32),
                pltpu.SemaphoreType.DMA((4,)),
            ],
            compiler_params=small,
        )(back)
        out = out.reshape(channels, count * outs // LANES, 2, LANES).transpose(0, 2, 1, 3)
        return out.reshape(channels, 2, count * outs)
    tiles = rows_out // SUB
    made = made.reshape(len(inner[0]), tiles, SUB, LANES).transpose(1, 0, 2, 3)
    made = made.reshape(tiles, count, sub, LANES).transpose(1, 0, 2, 3)
    back = exchange(made, range(count))
    full = outs // LANES
    head = back[:, : 8 * full].reshape(count, full, 4, 2, sub, LANES).transpose(4, 2, 3, 0, 1, 5)
    head = head.reshape(channels, 2, count, full * LANES)
    rest = back[:, 8 * full :].reshape(count, 4, sub, 2, outs - full * LANES).transpose(2, 1, 3, 0, 4)
    rest = rest.reshape(channels, 2, count, -1)
    return jnp.concatenate([head, rest], axis=3).reshape(channels, 2, count * outs)


def solution(mesh):
    in_specs = (P("tm", "station", None), P(), P())
    out_specs = P("tm", "station", None)
    orders = [list(range(mesh.shape["tm"]))] * 2
    if len(orders[0]) == len(ORDERS[0]):
        orders = ORDERS
    return jax.shard_map(
        functools.partial(shards, *orders),
        mesh=mesh,
        in_specs=in_specs,
        out_specs=out_specs,
        check_vma=False,
    )
```
